32 devices in a mesh: sub: 8 (over y, x, core), grp: 4 (over z).
Axes of the slice: x: 2, y: 2, z: 4, core: 2. Of those that a mesh axis runs over, the one named last changes fastest.
Arguments:
- impedance: bfloat16 [8, 4, 2048, 512], P('sub', 'grp'), may hold values from -0.125 to 0.125
- incident: bfloat16 [8, 4, 96, 512], P('sub', 'grp'), may hold values from -6 to 6
- face_order: int32 [8, 4, 192], P('sub', 'grp'), may hold values from 0 to 191, each once within a row
- near_tiles: bfloat16 [8, 4, 3, 128, 128], P('sub', 'grp'), may hold values from -0.3125 to 0.3125
- basis_right: bfloat16 [8, 4, 128, 128], P('sub', 'grp'), may hold values from -0.125 to 0.125
- rank_scale: float32 [8, 128], P('sub'), may hold values from 0.3 to 3
- rank_counts: int32 [2], replicated, may hold values from 32 to 128
- coupling: bfloat16 [8, 2, 128, 128], P('sub'), may hold values from -0.1875 to 0.1875
- basis_left: bfloat16 [8, 4, 128, 128], P('sub', 'grp'), may hold values from -0.5 to 0.5
Outputs:
- traces: bfloat16 [8, 4, 96, 512], P('sub', 'grp')
The draws below stay inside these ranges and needn't reach their ends.
Inputs may be any that keep to these rules, and one draw needn't show every extreme that they name: `face_order`: each row is a permutation of 0 to 191.
All inputs are finite; a program needn't handle non-finite values.
Results may differ from the reference program's by a relative error of at most 0.012.
Values may be sent and summed in bfloat16 or wider, within the bound.
A program may use at most 64 MiB of HBM per device.

```python
import math
from functools import partial
import jax
import jax.numpy as jnp
from jax import lax

ORDER = 2048
QUARTER = 512
FACE_Q = 192
OUTER_Q = 128
RANK = 128
EXC = 96
ITERS = 3
LAYERS = 2
N_SUB = 8
N_GRP = 4


def levels(own_key, extent, pieces, least, top_value):
    factor_of = 1.0
    for axis_at, shards_of in pieces:
        steps = jax.random.uniform(jax.random.fold_in(jax.random.fold_in(own_key, 6), axis_at), (shards_of,), jnp.float32, least / len(pieces), top_value / len(pieces))
        factor_of = factor_of * jnp.repeat(jnp.exp(steps), extent[axis_at] // shards_of).reshape((-1,) + (1,) * (len(extent) - 1 - axis_at))
    return factor_of


def normal_values(own_key, shape, deviation, most, pieces=(), held_as=jnp.bfloat16):
    level = levels(own_key, shape, pieces, -0.22, 0.18) if pieces else 1.0
    array = jax.random.normal(own_key, shape, jnp.float32) * deviation * level
    return jnp.minimum(jnp.maximum(array, -most), most).astype(held_as)


def setup_inputs(seed: int = 0) -> dict:
    arg_keys = jax.random.split(jax.random.key(seed), 10)
    impedance = normal_values(arg_keys[0], (N_SUB, N_GRP, ORDER, QUARTER), ORDER ** -0.5, 0.125, ((0, 8), (1, 4)))
    incident = normal_values(arg_keys[1], (N_SUB, N_GRP, EXC, QUARTER), 1.0, 6.0, ((0, 8), (1, 4)))
    face_order = jax.vmap(lambda own: jax.random.permutation(own, FACE_Q))(jax.random.split(arg_keys[2], N_SUB * N_GRP)).reshape((N_SUB, N_GRP, FACE_Q)).astype(jnp.int32)
    near_tiles = normal_values(arg_keys[3], (N_SUB, N_GRP, 3, OUTER_Q, OUTER_Q), (3 * OUTER_Q) ** -0.5, 0.3125, ((0, 8), (1, 4)))
    basis_right = normal_values(arg_keys[4], (N_SUB, N_GRP, OUTER_Q, RANK), (4 * N_GRP * OUTER_Q) ** -0.5, 0.125, ((0, 8), (1, 4)))
    rank_scale = jnp.clip(jnp.exp(math.log(3.0) - 2.3025851 * jax.random.uniform(arg_keys[5], (N_SUB, RANK), jnp.float32) ** levels(arg_keys[5], (N_SUB, RANK), ((0, 8),), -0.2, 0.2)), 0.3, 3.0)
    rank_counts = jax.random.randint(arg_keys[6], (LAYERS,), RANK // 4, RANK + 1).astype(jnp.int32)
    coupling = normal_values(arg_keys[7], (N_SUB, LAYERS, RANK, RANK), (RANK * N_SUB) ** -0.5, 0.1875, ((0, 8),))
    basis_left = normal_values(arg_keys[8], (N_SUB, N_GRP, RANK, OUTER_Q), RANK ** -0.5, 0.5, ((0, 8), (1, 4)))
    return dict(impedance=impedance, incident=incident, face_order=face_order, near_tiles=near_tiles, basis_right=basis_right, rank_scale=rank_scale, rank_counts=rank_counts, coupling=coupling, basis_left=basis_left)


def apply_layer(pair):
    whole, z_block = pair
    return jnp.einsum("gko,qgoc->qgkc", whole.astype(jnp.float32), z_block.astype(jnp.float32))


def far_target(coef_wide, owner, pair):
    couple_rows, mask_row = pair
    chosen = jnp.where(mask_row[:, None, None], couple_rows[owner].astype(jnp.float32), jnp.float32(0.0))
    return jnp.einsum("skr,srt->kt", coef_wide, chosen)


def reference(impedance, incident, face_order, near_tiles, basis_right, rank_scale, rank_counts, coupling, basis_left):
    layers = N_SUB // 4
    owner = (jnp.arange(N_SUB) // 4).astype(jnp.int32)
    kept = jnp.where(jnp.arange(RANK)[None, :] < rank_counts[owner][:, None], rank_scale, jnp.float32(0.0))
    far_mask = owner[:, None] != owner[None, :]
    z_layers = impedance.reshape(layers, 4, N_GRP, ORDER, QUARTER)
    trace_now = incident
    for sweep_index in range(ITERS):
        whole = trace_now.reshape(layers, 4, N_GRP, EXC, QUARTER).transpose(0, 2, 3, 1, 4).reshape(layers, N_GRP, EXC, ORDER)
        outgoing = lax.map(apply_layer, (whole, z_layers)).reshape(N_SUB, N_GRP, EXC, QUARTER).astype(jnp.bfloat16)
        lower_out = outgoing[..., :FACE_Q]
        upper_out = outgoing[..., FACE_Q:2 * FACE_Q]
        outer_out = outgoing[..., 2 * FACE_Q:]
        partial_sum = jnp.einsum("sgko,sgor->skr", outer_out.astype(jnp.float32), basis_right.astype(jnp.float32))
        coefs = (partial_sum * kept[:, None, :]).astype(jnp.bfloat16)
        coef_wide = coefs.astype(jnp.float32)
        far = lax.map(partial(far_target, coef_wide, owner), (coupling, far_mask)).astype(jnp.bfloat16)
        upper_below = jnp.concatenate([jnp.zeros_like(upper_out[:4]), upper_out[:-4]], 0)
        outer_below = jnp.concatenate([jnp.zeros_like(outer_out[:4]), outer_out[:-4]], 0)
        lower_above = jnp.concatenate([lower_out[4:], jnp.zeros_like(lower_out[:4])], 0)
        outer_above = jnp.concatenate([outer_out[4:], jnp.zeros_like(outer_out[:4])], 0)
        index_grid = jnp.broadcast_to(face_order[:, :, None, :], upper_below.shape).astype(jnp.int32)
        lower_in = jnp.take_along_axis(upper_below, index_grid, axis=3)
        tiles = near_tiles.astype(jnp.float32)
        outer_in = jnp.einsum("sgko,sgop->sgkp", outer_out.astype(jnp.float32), tiles[:, :, 0])
        outer_in = outer_in + jnp.einsum("sgko,sgop->sgkp", outer_below.astype(jnp.float32), tiles[:, :, 1])
        outer_in = outer_in + jnp.einsum("sgko,sgop->sgkp", outer_above.astype(jnp.float32), tiles[:, :, 2])
        outer_in = outer_in + jnp.einsum("skr,sgro->sgko", far.astype(jnp.float32), basis_left.astype(jnp.float32))
        joined = jnp.concatenate([lower_in.astype(jnp.float32), lower_above.astype(jnp.float32), outer_in], 3)
        trace_now = (joined + incident.astype(jnp.float32)).astype(jnp.bfloat16)
    return trace_now
```

```python
import functools
import jax
import jax.numpy as jnp
from jax import lax
from jax.experimental import pallas as pl
from jax.experimental.pallas import tpu as pltpu
from jax.sharding import PartitionSpec as P

FACE_Q = 192
ITERS = 3


def from_partner(value, axis, distance):
    mask = 2**distance
    pairs = [(source, source ^ mask) for source in range(lax.axis_size(axis))]
    return lax.ppermute(value, axis, pairs)


def shifted(value, axis, steps):
    count = lax.axis_size(axis)
    first, last = (max(0, -steps), min(count, count - steps))
    return lax.ppermute(value, axis, [(source, source + steps) for source in range(first, last)])


def per_device(
    impedance,
    incident,
    face_order,
    near_tiles,
    basis_right,
    rank_scale,
    rank_counts,
    coupling,
    basis_left,
):
    z_cols = impedance[0, 0]
    source = incident[0, 0]
    order_map = face_order[0, 0]
    tiles = near_tiles[0, 0]
    right_basis = basis_right[0, 0]
    left_basis = basis_left[0, 0]
    couple_rows = coupling[0]
    position = lax.axis_index("sub")
    cluster = position // 4
    rank_ids = jnp.arange(rank_scale.shape[1])
    kept = jnp.where(rank_ids < rank_counts[cluster], rank_scale[0], jnp.float32(0.0))
    trace_now = source
    for sweep_index in range(ITERS):
        whole = trace_now
        for bit_number in (0, 1):
            partner = from_partner(whole, "sub", bit_number)
            upper_half = position // (1 << bit_number) % 2 == 1
            whole = jnp.where(
                upper_half,
                jnp.concatenate([partner, whole], 1),
                jnp.concatenate([whole, partner], 1),
            )
        outgoing = jnp.dot(whole, z_cols, preferred_element_type=jnp.float32).astype(jnp.bfloat16)
        lower_out = outgoing[:, :FACE_Q]
        upper_out = outgoing[:, FACE_Q : 2 * FACE_Q]
        outer_out = outgoing[:, 2 * FACE_Q :]
        partial_sum = jnp.dot(outer_out, right_basis, preferred_element_type=jnp.float32)
        total = lax.psum(partial_sum.astype(jnp.bfloat16), "grp").astype(jnp.float32)
        coefs = (total * kept).astype(jnp.bfloat16)
        block_rows = lax.all_gather(coefs[None], "sub", axis=0, tiled=True)
        sources = jnp.arange(block_rows.shape[0]) // 4
        chosen = jnp.take(couple_rows, sources, axis=0)
        chosen = jnp.where((sources != cluster)[:, None, None], chosen, jnp.zeros_like(chosen))
        far = jnp.einsum(
            "nkr,nrt->kt", block_rows, chosen, preferred_element_type=jnp.float32
        ).astype(jnp.bfloat16)
        arrived = []
        for offset in (4, -4):
            sent = (upper_out, outer_out) if offset > 0 else (lower_out, outer_out)
            arrived.append(shifted((sent[0], sent[1]), "sub", offset))
        upper_below, outer_below = arrived[0]
        lower_above, outer_above = arrived[1]
        lower_in = jnp.take(upper_below, order_map, axis=1)
        outer_in = jnp.dot(outer_out, tiles[0], preferred_element_type=jnp.float32)
        outer_in = outer_in + jnp.dot(outer_below, tiles[1], preferred_element_type=jnp.float32)
        outer_in = outer_in + jnp.dot(outer_above, tiles[2], preferred_element_type=jnp.float32)
        outer_in = outer_in + jnp.dot(far, left_basis, preferred_element_type=jnp.float32)
        joined = jnp.concatenate(
            [lower_in.astype(jnp.float32), lower_above.astype(jnp.float32), outer_in], 1
        )
        trace_now = (joined + source.astype(jnp.float32)).astype(jnp.bfloat16)
    return trace_now[None, None]


QUARTERS = 4
F32 = jnp.float32
BF16 = jnp.bfloat16


def dot(a, b):
    return jnp.dot(a, b, preferred_element_type=F32)


def two_layer_kernel(
    groups,
    z_hbm,
    inc_hbm,
    order_hbm,
    tiles_hbm,
    right_hbm,
    scale_hbm,
    counts_hbm,
    couple_hbm,
    left_hbm,
    out_ref,
    inc_ref,
    order_ref,
    tiles_ref,
    right_ref,
    scale_ref,
    counts_ref,
    couple_ref,
    left_ref,
    z_ref,
    inc_all,
    order_all,
    pack_all,
    all_w,
    lhs,
    base,
    mine,
    own_outer,
    other,
    plane_sum,
    other_sum,
    z_sem,
    load_sem,
    const_send,
    const_recv,
    send,
    recv,
    far_send,
    far_recv,
):
    sub = lax.axis_index("sub")
    grp = lax.axis_index("grp")
    layer = sub // QUARTERS
    q = sub % QUARTERS
    exc, width = inc_ref.shape
    half = exc // 2
    rank = right_ref.shape[1]
    outer = tiles_ref.shape[1]
    face = order_ref.shape[1]
    upper = layer == 1
    flip0 = sub + 1 - 2 * (sub % 2)
    flip1 = sub + 2 - 4 * ((sub // 2) % 2)
    flip2 = sub + 4 - 8 * layer
    flip12 = flip1 + 4 - 8 * layer
    q1 = flip0 % QUARTERS
    q2 = flip1 % QUARTERS
    q3 = (flip1 + 1 - 2 * (flip1 % 2)) % QUARTERS

    def remote(src, dst, send_sem, recv_sem, to_sub, to_grp=None):
        return pltpu.make_async_remote_copy(
            src_ref=src,
            dst_ref=dst,
            send_sem=send_sem,
            recv_sem=recv_sem,
            device_id=(to_sub, grp if to_grp is None else to_grp),
            device_id_type=pl.DeviceIdType.MESH,
        )

    loads = []
    pairs = [
        (right_hbm, right_ref),
        (scale_hbm, scale_ref),
        (counts_hbm, counts_ref),
        (tiles_hbm, tiles_ref),
        (couple_hbm, couple_ref),
        (left_hbm, left_ref),
        (inc_hbm, inc_ref),
        (order_hbm, order_ref),
    ]
    for i, (src, dst) in enumerate(pairs):
        load = pltpu.make_async_copy(src, dst, load_sem.at[i])
        load.start()
        loads.append(load)
    z_copies = []
    for part in range(QUARTERS):
        rows = pl.ds(part * width, width)
        copy = pltpu.make_async_copy(z_hbm.at[rows], z_ref.at[rows], z_sem.at[part])
        copy.start()
        z_copies.append(copy)

    barrier = pltpu.get_barrier_semaphore()
    greet = [(flip0, grp), (flip1, grp), (flip2, grp), (flip12, grp)]
    greet += [(flip2, lax.rem(grp + d, groups)) for d in range(1, groups)]
    for device in greet:
        pl.semaphore_signal(barrier, inc=1, device_id=device, device_id_type=pl.DeviceIdType.MESH)

    for load in loads:
        load.wait()
    lanes = lax.broadcasted_iota(jnp.int32, (1, rank), 1)
    kept = jnp.where(lanes < counts_ref[layer], scale_ref[...], F32(0.0))
    pack_all[q, 0:outer] = (right_ref[...].astype(F32) * kept).astype(BF16)
    pack_all[q, outer : 2 * outer] = tiles_ref[0]
    pack_all[q, 2 * outer : 3 * outer] = tiles_ref[2 - layer]
    left_map = dot(couple_ref[1 - layer], left_ref[...]).astype(BF16)
    pack_all[q, 3 * outer : 3 * outer + rank] = left_map
    inc_all[q] = inc_ref[...]
    order_all[q] = order_ref[...]
    pl.semaphore_wait(barrier, len(greet))

    pending = []
    kinds = [(inc_all, inc_ref, 0), (pack_all, pack_all.at[q], 1), (order_all, order_ref, 2)]
    firsts = []
    for buf, src, i in kinds:
        a = remote(src, buf.at[q], const_send.at[i, 0], const_recv.at[i, 0], flip1)
        b = remote(src, buf.at[q], const_send.at[i, 1], const_recv.at[i, 1], flip0)
        a.start()
        b.start()
        firsts.append((a, b))
        pending += [a, b]

    def const_forward(i):
        buf = kinds[i][0]
        firsts[i][0].wait_recv()
        c = remote(buf.at[q2], buf.at[q2], const_send.at[i, 2], const_recv.at[i, 2], flip0)
        c.start()
        pending.append(c)
        return c

    for copy in z_copies:
        copy.wait()
    def z_quarter(index):
        return z_ref[pl.ds(pl.multiple_of(index * width, width), width), :]

    acc = dot(inc_ref[...], z_quarter(q))
    firsts[0][1].wait_recv()
    acc = acc + dot(inc_all[q1], z_quarter(q1))
    fwd = const_forward(0)
    acc = acc + dot(inc_all[q2], z_quarter(q2))
    fwd.wait_recv()
    acc = acc + dot(inc_all[q3], z_quarter(q3))
    base[...] = acc

    lane = lax.broadcasted_iota(jnp.int32, (half, outer), 1)
    low = lane < outer // 2
    first_here = low == upper
    first_there = low != upper
    slot = lax.broadcasted_iota(jnp.int32, (2 * outer, 2 * face), 0)
    in_half = slot % (outer // 2)
    full_entry = jnp.where(upper, slot + outer // 2, slot)
    half_entry = jnp.where(upper, in_half, in_half + outer)
    entry = jnp.where(slot < outer, full_entry, half_entry)
    along = lax.broadcasted_iota(jnp.int32, (1, face), 1)
    nothing = jnp.full((1, face), -1, jnp.int32)

    def chosen(order_row):
        below = jnp.where(upper, order_row, nothing)
        above = jnp.where(upper, nothing, along)
        wanted = jnp.concatenate([below, above], 1)
        return jnp.where(entry == wanted, F32(1.0), F32(0.0)).astype(BF16)

    def face_tiles(block):
        full = block[exc : 2 * exc]
        packed = block[2 * exc : 2 * exc + half]
        zero = jnp.zeros_like(packed)
        top = jnp.where(first_there, packed, zero)
        bottom = jnp.where(first_there, zero, packed)
        return jnp.concatenate([full, jnp.concatenate([top, bottom], 0)], 1)

    def weights():
        for part in range(QUARTERS):
            start = part * width
            z_outer = z_ref[start + 2 * face : start + width, :]
            pack = pack_all[part]
            made = dot(pack[outer:], z_outer)
            all_w[part * outer : (part + 1) * outer, :] = made[:outer].astype(BF16)
            at = (QUARTERS + 3 * part) * outer
            all_w[at : at + outer, :] = made[outer : 2 * outer].astype(BF16)
            term = made[2 * outer :]
            total = term if part == 0 else total + term
            z_face = z_ref[start : start + 2 * face, :]
            all_w[at + outer : at + 3 * outer, :] = dot(chosen(order_all[part]), z_face).astype(BF16)
        at = 4 * QUARTERS * outer
        all_w[at : at + rank, :] = total.astype(BF16)
        all_w[at + rank :, :] = jnp.zeros_like(all_w[at + rank :, :])
        lhs[:, at + rank :] = jnp.zeros_like(lhs[:, at + rank :])

    for sweep in range(ITERS):
        last = sweep == ITERS - 1
        y = acc.astype(BF16)
        outer_out = y[:, 2 * face :]
        mid = acc[:, outer : 2 * outer]
        rolled = pltpu.roll(mid, outer // 2, 1)
        mine[sweep, 0:exc] = outer_out
        mine[sweep, exc : 2 * exc] = jnp.where(upper, acc[:, 0:outer], acc[:, 2 * outer : 3 * outer]).astype(BF16)
        mine[sweep, 2 * exc : 2 * exc + half] = jnp.where(first_here, mid[:half], rolled[half:]).astype(BF16)
        own_outer[sweep, q] = outer_out

        ss, rs = send.at[sweep], recv.at[sweep]
        o_x = remote(mine.at[sweep, pl.ds(0, exc)], own_outer.at[sweep, q], ss.at[2], rs.at[2], flip1)
        o_c = remote(mine.at[sweep, pl.ds(0, exc)], own_outer.at[sweep, q], ss.at[3], rs.at[3], flip0)
        w_y = remote(mine.at[sweep], other.at[sweep, q], ss.at[0], rs.at[0], flip2)
        o_x.start()
        o_c.start()
        w_y.start()
        pending += [o_x, o_c, w_y]
        if not last:
            w_d = remote(mine.at[sweep], other.at[sweep, q], ss.at[1], rs.at[1], flip12)
            w_d.start()
            pending.append(w_d)

        if sweep == 0:
            consts = [const_forward(1), const_forward(2)]
            for i in (1, 2):
                firsts[i][1].wait_recv()
            for c in consts:
                c.wait_recv()

        o_x.wait_recv()
        o_f = remote(own_outer.at[sweep, q2], own_outer.at[sweep, q2], ss.at[4], rs.at[4], flip0)
        o_f.start()
        pending.append(o_f)
        o_c.wait_recv()
        o_f.wait_recv()
        outers = jnp.concatenate([own_outer[sweep, part] for part in range(QUARTERS)], 1)
        rights = jnp.concatenate([pack_all[part, 0:outer] for part in range(QUARTERS)], 0)
        plane_sum[sweep] = dot(outers, rights).astype(BF16)
        sums = []
        for d in range(groups):
            copy = remote(
                plane_sum.at[sweep],
                other_sum.at[sweep, d],
                far_send.at[sweep, d],
                far_recv.at[sweep, d],
                flip2,
                lax.rem(grp + d, groups),
            )
            copy.start()
            sums.append(copy)
        pending += sums

        if sweep == 0:
            weights()
        if not last:
            lhs[:, 0 : QUARTERS * outer] = outers
            w_y.wait_recv()
            y_f = remote(other.at[sweep, q], other.at[sweep, q], ss.at[5], rs.at[5], flip0)
            y_f.start()
            w_d.wait_recv()
            d_f = remote(other.at[sweep, q2], other.at[sweep, q2], ss.at[6], rs.at[6], flip0)
            d_f.start()
            pending += [y_f, d_f]
            y_f.wait_recv()
            d_f.wait_recv()
            for part in range(QUARTERS):
                at = (QUARTERS + 3 * part) * outer
                block = other[sweep, part]
                lhs[:, at : at + outer] = block[:exc]
                lhs[:, at + outer : at + 3 * outer] = face_tiles(block)
        else:
            w_y.wait_recv()
            block = other[sweep, q]
            outer_in = dot(outer_out, tiles_ref[0]) + dot(block[:exc], tiles_ref[2 - layer])
            faces = dot(face_tiles(block), chosen(order_ref[...]))
            inc = inc_ref[...].astype(F32)
            faces = faces + inc[:, : 2 * face]
            outer_in = outer_in + inc[:, 2 * face :]

        for copy in sums:
            copy.wait_recv()
        total = other_sum[sweep, 0].astype(F32)
        for d in range(1, groups):
            total = total + other_sum[sweep, d].astype(F32)
        total = total.astype(BF16)
        if not last:
            at = 4 * QUARTERS * outer
            lhs[:, at : at + rank] = total
            acc = base[...] + dot(lhs[...], all_w[...])
        else:
            outer_in = outer_in + dot(total, pack_all[q, 3 * outer : 3 * outer + rank])
            out_ref[...] = jnp.concatenate([faces, outer_in], 1).astype(BF16)
    for copy in pending:
        copy.wait_send()


def two_layers(
    groups,
    impedance,
    incident,
    face_order,
    near_tiles,
    basis_right,
    rank_scale,
    rank_counts,
    coupling,
    basis_left,
):
    order, width = impedance.shape[2:]
    exc = incident.shape[2]
    face = face_order.shape[2]
    outer = near_tiles.shape[3]
    rank = basis_right.shape[3]
    vmem = pl.BlockSpec(memory_space=pltpu.VMEM)
    dma = pltpu.SemaphoreType.DMA
    block = 2 * exc + exc // 2
    out = pl.pallas_call(
        functools.partial(two_layer_kernel, groups),
        out_shape=jax.ShapeDtypeStruct((exc, width), BF16),
        in_specs=[pl.BlockSpec(memory_space=pltpu.HBM)] * 9,
        out_specs=vmem,
        scratch_shapes=[
            pltpu.VMEM((exc, width), BF16),
            pltpu.VMEM((1, face), jnp.int32),
            pltpu.VMEM(near_tiles.shape[2:], BF16),
            pltpu.VMEM(basis_right.shape[2:], BF16),
            pltpu.VMEM((1, rank), F32),
            pltpu.SMEM(rank_counts.shape, jnp.int32),
            pltpu.VMEM(coupling.shape[1:], BF16),
            pltpu.VMEM(basis_left.shape[2:], BF16),
            pltpu.VMEM((order, width), BF16),
            pltpu.VMEM((QUARTERS, exc, width), BF16),
            pltpu.VMEM((QUARTERS, 1, face), jnp.int32),
            pltpu.VMEM((QUARTERS, 3 * outer + rank, outer), BF16),
            pltpu.VMEM((4 * QUARTERS * outer + 2 * rank, width), BF16),
            pltpu.VMEM((exc, 4 * QUARTERS * outer + 2 * rank), BF16),
            pltpu.VMEM((exc, width), F32),
            pltpu.VMEM((ITERS, block, outer), BF16),
            pltpu.VMEM((ITERS, QUARTERS, exc, outer), BF16),
            pltpu.VMEM((ITERS, QUARTERS, block, outer), BF16),
            pltpu.VMEM((ITERS, exc, rank), BF16),
            pltpu.VMEM((ITERS, groups, exc, rank), BF16),
            dma((QUARTERS,)),
            dma((8,)),
            dma((3, 3)),
            dma((3, 3)),
            dma((ITERS, 7)),
            dma((ITERS, 7)),
            dma((ITERS, groups)),
            dma((ITERS, groups)),
        ],
        compiler_params=pltpu.CompilerParams(
            collective_id=0, has_side_effects=True, vmem_limit_bytes=48 * 1024 * 1024
        ),
    )(
        *[
            pltpu.with_memory_space_constraint(operand, pltpu.HBM)
            for operand in (
                impedance[0, 0],
                incident[0, 0],
                face_order[0],
                near_tiles[0, 0],
                basis_right[0, 0],
                rank_scale,
                rank_counts,
                coupling[0],
                basis_left[0, 0],
            )
        ]
    )
    return out[None, None]


def solution(mesh):
    placed = (
        P("sub", "grp", None, None),
        P("sub", "grp", None, None),
        P("sub", "grp", None),
        P("sub", "grp", None, None, None),
        P("sub", "grp", None, None),
        P("sub", None),
        P(),
        P("sub", None, None, None),
        P("sub", "grp", None, None),
    )
    two = mesh.shape["sub"] == 2 * QUARTERS
    body = functools.partial(two_layers, mesh.shape["grp"]) if two else per_device
    return jax.shard_map(
        body,
        mesh=mesh,
        in_specs=placed,
        out_specs=P("sub", "grp", None, None),
        check_vma=False,
    )
```

```python
import functools
import jax
import jax.numpy as jnp
from jax import lax
from jax.experimental import pallas as pl
from jax.experimental.pallas import tpu as pltpu
from jax.sharding import PartitionSpec as P

FACE_Q = 192
ITERS = 3


def from_partner(value, axis, distance):
    mask = 2**distance
    pairs = [(source, source ^ mask) for source in range(lax.axis_size(axis))]
    return lax.ppermute(value, axis, pairs)


def shifted(value, axis, steps):
    count = lax.axis_size(axis)
    first, last = (max(0, -steps), min(count, count - steps))
    return lax.ppermute(value, axis, [(source, source + steps) for source in range(first, last)])


def per_device(
    impedance,
    incident,
    face_order,
    near_tiles,
    basis_right,
    rank_scale,
    rank_counts,
    coupling,
    basis_left,
):
    z_cols = impedance[0, 0]
    source = incident[0, 0]
    order_map = face_order[0, 0]
    tiles = near_tiles[0, 0]
    right_basis = basis_right[0, 0]
    left_basis = basis_left[0, 0]
    couple_rows = coupling[0]
    position = lax.axis_index("sub")
    cluster = position // 4
    rank_ids = jnp.arange(rank_scale.shape[1])
    kept = jnp.where(rank_ids < rank_counts[cluster], rank_scale[0], jnp.float32(0.0))
    trace_now = source
    for sweep_index in range(ITERS):
        whole = trace_now
        for bit_number in (0, 1):
            partner = from_partner(whole, "sub", bit_number)
            upper_half = position // (1 << bit_number) % 2 == 1
            whole = jnp.where(
                upper_half,
                jnp.concatenate([partner, whole], 1),
                jnp.concatenate([whole, partner], 1),
            )
        outgoing = jnp.dot(whole, z_cols, preferred_element_type=jnp.float32).astype(jnp.bfloat16)
        lower_out = outgoing[:, :FACE_Q]
        upper_out = outgoing[:, FACE_Q : 2 * FACE_Q]
        outer_out = outgoing[:, 2 * FACE_Q :]
        partial_sum = jnp.dot(outer_out, right_basis, preferred_element_type=jnp.float32)
        total = lax.psum(partial_sum.astype(jnp.bfloat16), "grp").astype(jnp.float32)
        coefs = (total * kept).astype(jnp.bfloat16)
        block_rows = lax.all_gather(coefs[None], "sub", axis=0, tiled=True)
        sources = jnp.arange(block_rows.shape[0]) // 4
        chosen = jnp.take(couple_rows, sources, axis=0)
        chosen = jnp.where((sources != cluster)[:, None, None], chosen, jnp.zeros_like(chosen))
        far = jnp.einsum(
            "nkr,nrt->kt", block_rows, chosen, preferred_element_type=jnp.float32
        ).astype(jnp.bfloat16)
        arrived = []
        for offset in (4, -4):
            sent = (upper_out, outer_out) if offset > 0 else (lower_out, outer_out)
            arrived.append(shifted((sent[0], sent[1]), "sub", offset))
        upper_below, outer_below = arrived[0]
        lower_above, outer_above = arrived[1]
        lower_in = jnp.take(upper_below, order_map, axis=1)
        outer_in = jnp.dot(outer_out, tiles[0], preferred_element_type=jnp.float32)
        outer_in = outer_in + jnp.dot(outer_below, tiles[1], preferred_element_type=jnp.float32)
        outer_in = outer_in + jnp.dot(outer_above, tiles[2], preferred_element_type=jnp.float32)
        outer_in = outer_in + jnp.dot(far, left_basis, preferred_element_type=jnp.float32)
        joined = jnp.concatenate(
            [lower_in.astype(jnp.float32), lower_above.astype(jnp.float32), outer_in], 1
        )
        trace_now = (joined + source.astype(jnp.float32)).astype(jnp.bfloat16)
    return trace_now[None, None]


QUARTERS = 4
F32 = jnp.float32
BF16 = jnp.bfloat16


def dot(a, b):
    return jnp.dot(a, b, preferred_element_type=F32)


def two_layer_kernel(
    groups,
    z_hbm,
    inc_hbm,
    order_hbm,
    tiles_hbm,
    right_hbm,
    scale_hbm,
    counts_hbm,
    couple_hbm,
    left_hbm,
    out_ref,
    tiles_ref,
    right_ref,
    scale_ref,
    counts_ref,
    couple_ref,
    left_ref,
    z_ref,
    inc_all,
    order_all,
    right_all,
    pack_all,
    all_w,
    g_all,
    base,
    mine,
    own_outer,
    other,
    plane_sum,
    other_sum,
    z_sem,
    load_sem,
    const_send,
    const_recv,
    send,
    recv,
    far_send,
    far_recv,
    g_send,
    g_recv,
    slab_sem,
    ready_sem,
    go_sem,
):
    sub = lax.axis_index("sub")
    grp = lax.axis_index("grp")
    layer = sub // QUARTERS
    q = sub % QUARTERS
    exc, width = inc_all.shape[1:]
    half = exc // 2
    rank = right_ref.shape[1]
    outer = tiles_ref.shape[1]
    face = order_all.shape[2]
    upper = layer == 1
    flip0 = sub + 1 - 2 * (sub % 2)
    flip1 = sub + 2 - 4 * ((sub // 2) % 2)
    flip01 = flip1 + 1 - 2 * (flip1 % 2)
    flip2 = sub + 4 - 8 * layer
    flip12 = flip1 + 4 - 8 * layer
    q1 = flip0 % QUARTERS
    q2 = flip1 % QUARTERS
    q3 = flip01 % QUARTERS

    def remote(src, dst, send_sem, recv_sem, to_sub, to_grp=None):
        return pltpu.make_async_remote_copy(
            src_ref=src,
            dst_ref=dst,
            send_sem=send_sem,
            recv_sem=recv_sem,
            device_id=(to_sub, grp if to_grp is None else to_grp),
            device_id_type=pl.DeviceIdType.MESH,
        )

    def signal(sem, to_sub, to_grp):
        pl.semaphore_signal(
            sem, inc=1, device_id=(to_sub, to_grp), device_id_type=pl.DeviceIdType.MESH
        )

    loads = {}
    for i, (name, src, dst) in enumerate(
        [
            ("inc", inc_hbm, inc_all.at[q]),
            ("right", right_hbm, right_ref),
            ("scale", scale_hbm, scale_ref),
            ("counts", counts_hbm, counts_ref),
            ("couple", couple_hbm, couple_ref),
            ("left", left_hbm, left_ref),
            ("tiles", tiles_hbm, tiles_ref),
            ("own", tiles_hbm.at[0], pack_all.at[q, pl.ds(0, outer)]),
            ("cross", tiles_hbm.at[2 - layer], pack_all.at[q, pl.ds(outer, outer)]),
            ("order", order_hbm, order_all.at[q]),
        ]
    ):
        loads[name] = pltpu.make_async_copy(src, dst, load_sem.at[i])
        loads[name].start()
    z_copies = []
    for part in range(QUARTERS):
        rows = pl.ds(part * width, width)
        copy = pltpu.make_async_copy(z_hbm.at[rows], z_ref.at[rows], z_sem.at[part])
        copy.start()
        z_copies.append(copy)

    slab = 2 * QUARTERS
    lead = sub == 0
    barrier = pltpu.get_barrier_semaphore()

    @pl.when(lead)
    def _():
        for i in range(1, slab):
            signal(barrier, i, grp)
        for d in range(1, groups):
            signal(barrier, sub, lax.rem(grp + d, groups))

    @pl.when(jnp.logical_not(lead))
    def _():
        for i in range(1, slab - 1):
            signal(barrier, 1 + lax.rem(sub - 1 + i, slab - 1), grp)
        pl.semaphore_wait(barrier, slab - 1)
        signal(slab_sem, 0, grp)

    @pl.when(lead)
    def _():
        pl.semaphore_wait(slab_sem, slab - 1)

    pending = []
    buffers = [inc_all, right_all, pack_all, order_all]
    firsts = {}

    def const_start(i):
        buf = buffers[i]
        a = remote(buf.at[q], buf.at[q], const_send.at[i, 0], const_recv.at[i, 0], flip1)
        b = remote(buf.at[q], buf.at[q], const_send.at[i, 1], const_recv.at[i, 1], flip0)
        a.start()
        b.start()
        firsts[i] = (a, b)
        pending.extend([a, b])

    def const_forward(i):
        buf = buffers[i]
        firsts[i][0].wait_recv()
        c = remote(buf.at[q2], buf.at[q2], const_send.at[i, 2], const_recv.at[i, 2], flip0)
        c.start()
        pending.append(c)
        return c

    loads["inc"].wait()
    const_start(0)

    for name in ("right", "scale", "counts"):
        loads[name].wait()
    lanes = lax.broadcasted_iota(jnp.int32, (1, rank), 1)
    kept = jnp.where(lanes < counts_ref[layer], scale_ref[...], F32(0.0))
    right_all[q] = (right_ref[...].astype(F32) * kept).astype(BF16)

    for name in ("couple", "left", "tiles", "own", "cross", "order"):
        loads[name].wait()
    left_map = dot(couple_ref[1 - layer], left_ref[...]).astype(BF16)
    pack_all[q, 2 * outer : 2 * outer + rank] = left_map

    @pl.when(lead)
    def _():
        pl.semaphore_wait(barrier, groups - 1)
        for d in range(1, groups):
            signal(ready_sem, sub, lax.rem(grp + d, groups))

    for copy in z_copies:
        copy.wait()

    def z_quarter(index):
        return z_ref[pl.ds(pl.multiple_of(index * width, width), width), :]

    acc = dot(inc_all[q], z_quarter(q))
    firsts[0][1].wait_recv()
    acc = acc + dot(inc_all[q1], z_quarter(q1))
    for i in (1, 2, 3):
        const_start(i)

    @pl.when(lead)
    def _():
        pl.semaphore_wait(ready_sem, groups - 1)
        for i in range(1, slab):
            signal(go_sem, i, grp)

    fwd = const_forward(0)
    acc = acc + dot(inc_all[q2], z_quarter(q2))
    right_fwd = const_forward(1)
    fwd.wait_recv()
    acc = acc + dot(inc_all[q3], z_quarter(q3))
    base[...] = acc

    lane = lax.broadcasted_iota(jnp.int32, (half, outer), 1)
    low = lane < outer // 2
    first_here = low == upper
    first_there = low != upper
    slot = lax.broadcasted_iota(jnp.int32, (2 * outer, 2 * face), 0)
    in_half = slot % (outer // 2)
    full_entry = jnp.where(upper, slot + outer // 2, slot)
    half_entry = jnp.where(upper, in_half, in_half + outer)
    entry = jnp.where(slot < outer, full_entry, half_entry)
    along = lax.broadcasted_iota(jnp.int32, (1, face), 1)
    nothing = jnp.full((1, face), -1, jnp.int32)
    far_at = 4 * QUARTERS * outer

    def chosen(order_row):
        below = jnp.where(upper, order_row, nothing)
        above = jnp.where(upper, nothing, along)
        wanted = jnp.concatenate([below, above], 1)
        return jnp.where(entry == wanted, F32(1.0), F32(0.0)).astype(BF16)

    def face_tiles(block):
        full = block[exc : 2 * exc]
        packed = block[2 * exc : 2 * exc + half]
        zero = jnp.zeros_like(packed)
        top = jnp.where(first_there, packed, zero)
        bottom = jnp.where(first_there, zero, packed)
        return jnp.concatenate([full, jnp.concatenate([top, bottom], 0)], 1)

    def weights():
        for part in range(QUARTERS):
            start = part * width
            z_outer = z_ref[start + 2 * face : start + width, :]
            made = dot(pack_all[part], z_outer)
            all_w[part * outer : (part + 1) * outer, :] = made[:outer].astype(BF16)
            at = (QUARTERS + 3 * part) * outer
            all_w[at : at + outer, :] = made[outer : 2 * outer].astype(BF16)
            term = made[2 * outer :]
            total = term if part == 0 else total + term
            z_face = z_ref[start : start + 2 * face, :]
            all_w[at + outer : at + 3 * outer, :] = dot(chosen(order_all[part]), z_face).astype(BF16)
        all_w[far_at : far_at + rank, :] = total.astype(BF16)

    def start_outer(sweep, outer_out):
        own_outer[sweep, q] = outer_out
        own_at = own_outer.at[sweep, q]
        ss, rs = send.at[sweep], recv.at[sweep]
        o_c = remote(own_at, own_at, ss.at[3], rs.at[3], flip0)
        o_x = remote(own_at, own_at, ss.at[2], rs.at[2], flip1)
        o_d = remote(own_at, own_at, ss.at[4], rs.at[4], flip01)
        for copy in (o_d, o_x, o_c):
            copy.start()
            pending.append(copy)
        return o_c, o_x, o_d

    def start_near(sweep, acc):
        ss, rs = send.at[sweep], recv.at[sweep]
        mid = acc[:, outer : 2 * outer]
        rolled = pltpu.roll(mid, outer // 2, 1)
        mine[sweep, 0:exc] = acc[:, 2 * face :].astype(BF16)
        mine[sweep, exc : 2 * exc] = jnp.where(upper, acc[:, 0:outer], acc[:, 2 * outer : 3 * outer]).astype(BF16)
        mine[sweep, 2 * exc : 2 * exc + half] = jnp.where(first_here, mid[:half], rolled[half:]).astype(BF16)
        w_y = remote(mine.at[sweep], other.at[sweep, q], ss.at[0], rs.at[0], flip2)
        copies = [w_y]
        if sweep < ITERS - 1:
            copies.append(remote(mine.at[sweep], other.at[sweep, q], ss.at[1], rs.at[1], flip12))
        for copy in copies:
            copy.start()
            pending.append(copy)
        return copies

    def outer_pair(sweep, first, second):
        return dot(
            jnp.concatenate([own_outer[sweep, first], own_outer[sweep, second]], 1),
            jnp.concatenate([right_all[first], right_all[second]], 0),
        )

    def start_sums(sweep, value):
        plane_sum[sweep] = value.astype(BF16)
        sums = []
        for d in sorted(range(groups), key=lambda d: -min(d, groups - d)):
            copy = remote(
                plane_sum.at[sweep],
                other_sum.at[sweep, d],
                far_send.at[sweep, d],
                far_recv.at[sweep, d],
                flip2,
                lax.rem(grp + d, groups),
            )
            copy.start()
            sums.append(copy)
            pending.append(copy)
        return sums

    def far_total(sweep, sums):
        for copy in sums:
            copy.wait_recv()
        total = other_sum[sweep, 0].astype(F32)
        for d in range(1, groups):
            total = total + other_sum[sweep, d].astype(F32)
        return total.astype(BF16)

    def near_block(sweep, part):
        block = other[sweep, part]
        return jnp.concatenate([block[:exc], face_tiles(block)], 1)

    def near_rows(part):
        at = pl.multiple_of((QUARTERS + 3 * part) * outer, outer)
        return all_w[pl.ds(at, 3 * outer), :]

    def known_terms(sweep, w_y, w_d):
        ss, rs = send.at[sweep], recv.at[sweep]
        y_f = remote(other.at[sweep, q], other.at[sweep, q], ss.at[5], rs.at[5], flip0)
        d_f = remote(other.at[sweep, q2], other.at[sweep, q2], ss.at[6], rs.at[6], flip0)
        pending.extend([y_f, d_f])
        outers = jnp.concatenate([own_outer[sweep, part] for part in range(QUARTERS)], 1)
        known = base[...] + dot(outers, all_w[0 : QUARTERS * outer, :])
        w_y.wait_recv()
        y_f.start()
        known = known + dot(near_block(sweep, q), near_rows(q))
        w_d.wait_recv()
        d_f.start()
        known = known + dot(near_block(sweep, q2), near_rows(q2))
        y_f.wait_recv()
        known = known + dot(near_block(sweep, q1), near_rows(q1))
        d_f.wait_recv()
        block, rows = near_block(sweep, q3), near_rows(q3)
        ahead = None
        known_outer = known[:, 2 * face :] + dot(block, rows[:, 2 * face :])
        if sweep == ITERS - 2:
            ahead = start_outer(sweep + 1, known_outer.astype(BF16))
        known_face = known[:, : 2 * face] + dot(block, rows[:, : 2 * face])
        return jnp.concatenate([known_face, known_outer], 1), ahead

    for sweep in range(ITERS):
        last = sweep == ITERS - 1
        if sweep == 0:
            outs = start_outer(sweep, acc[:, 2 * face :].astype(BF16))
            near = start_near(sweep, acc)
            consts = [const_forward(2), const_forward(3)]
            firsts[1][1].wait_recv()
        elif not last:
            near = start_near(sweep, acc)
            outs = start_outer(sweep, acc[:, 2 * face :].astype(BF16))
        else:
            near = start_near(sweep, acc)
            outs = ahead
        outs[0].wait_recv()
        value = outer_pair(sweep, q, q1)
        if last:
            for copy in shares:
                copy.wait_recv()
            whole = g_all[0].astype(F32)
            for part in range(1, QUARTERS):
                whole = whole + g_all[part].astype(F32)
            value = value + dot(total, whole.astype(BF16))
        if sweep == 0:
            right_fwd.wait_recv()
        outs[1].wait_recv()
        outs[2].wait_recv()
        value = value + outer_pair(sweep, q2, q3)
        if sweep == 0:

            @pl.when(jnp.logical_not(lead))
            def _():
                pl.semaphore_wait(go_sem, 1)

        sums = start_sums(sweep, value)
        if sweep == 0:
            for i in (2, 3):
                firsts[i][1].wait_recv()
            for c in consts:
                c.wait_recv()
            weights()
            far_outer = all_w[far_at : far_at + rank, 2 * face :]
            g_all[q] = dot(far_outer, right_all[q]).astype(BF16)
            shares = [
                remote(g_all.at[q], g_all.at[q], g_send.at[i], g_recv.at[i], peer)
                for i, peer in enumerate((flip01, flip1, flip0))
            ]
            for copy in shares:
                copy.start()
                pending.append(copy)
        if not last:
            known, ahead = known_terms(sweep, *near)
            total = far_total(sweep, sums)
            acc = known + dot(total, all_w[far_at : far_at + rank, :])
        else:
            near[0].wait_recv()
            block = other[sweep, q]
            outer_in = dot(acc[:, 2 * face :].astype(BF16), tiles_ref[0])
            outer_in = outer_in + dot(block[:exc], tiles_ref[2 - layer])
            faces = dot(face_tiles(block), chosen(order_all[q]))
            inc = inc_all[q].astype(F32)
            out_ref[:, 0 : 2 * face] = (faces + inc[:, : 2 * face]).astype(BF16)
            outer_in = outer_in + inc[:, 2 * face :]
            total = far_total(sweep, sums)
            outer_in = outer_in + dot(total, pack_all[q, 2 * outer : 2 * outer + rank])
            out_ref[:, 2 * face :] = outer_in.astype(BF16)
    for copy in pending:
        copy.wait_send()


def two_layers(
    groups,
    impedance,
    incident,
    face_order,
    near_tiles,
    basis_right,
    rank_scale,
    rank_counts,
    coupling,
    basis_left,
):
    order, width = impedance.shape[2:]
    exc = incident.shape[2]
    face = face_order.shape[2]
    outer = near_tiles.shape[3]
    rank = basis_right.shape[3]
    vmem = pl.BlockSpec(memory_space=pltpu.VMEM)
    dma = pltpu.SemaphoreType.DMA
    block = 2 * exc + exc // 2
    out = pl.pallas_call(
        functools.partial(two_layer_kernel, groups),
        out_shape=jax.ShapeDtypeStruct((exc, width), BF16),
        in_specs=[pl.BlockSpec(memory_space=pltpu.HBM)] * 9,
        out_specs=vmem,
        scratch_shapes=[
            pltpu.VMEM(near_tiles.shape[2:], BF16),
            pltpu.VMEM(basis_right.shape[2:], BF16),
            pltpu.VMEM((1, rank), F32),
            pltpu.SMEM(rank_counts.shape, jnp.int32),
            pltpu.VMEM(coupling.shape[1:], BF16),
            pltpu.VMEM(basis_left.shape[2:], BF16),
            pltpu.VMEM((order, width), BF16),
            pltpu.VMEM((QUARTERS, exc, width), BF16),
            pltpu.VMEM((QUARTERS, 1, face), jnp.int32),
            pltpu.VMEM((QUARTERS, outer, rank), BF16),
            pltpu.VMEM((QUARTERS, 2 * outer + rank, outer), BF16),
            pltpu.VMEM((4 * QUARTERS * outer + rank, width), BF16),
            pltpu.VMEM((QUARTERS, rank, rank), BF16),
            pltpu.VMEM((exc, width), F32),
            pltpu.VMEM((ITERS, block, outer), BF16),
            pltpu.VMEM((ITERS, QUARTERS, exc, outer), BF16),
            pltpu.VMEM((ITERS, QUARTERS, block, outer), BF16),
            pltpu.VMEM((ITERS, exc, rank), BF16),
            pltpu.VMEM((ITERS, groups, exc, rank), BF16),
            dma((QUARTERS,)),
            dma((10,)),
            dma((4, 3)),
            dma((4, 3)),
            dma((ITERS, 7)),
            dma((ITERS, 7)),
            dma((ITERS, groups)),
            dma((ITERS, groups)),
            dma((3,)),
            dma((3,)),
            pltpu.SemaphoreType.REGULAR,
            pltpu.SemaphoreType.REGULAR,
            pltpu.SemaphoreType.REGULAR,
        ],
        compiler_params=pltpu.CompilerParams(
            collective_id=0, has_side_effects=True, vmem_limit_bytes=48 * 1024 * 1024
        ),
    )(
        *[
            pltpu.with_memory_space_constraint(operand, pltpu.HBM)
            for operand in (
                impedance[0, 0],
                incident[0, 0],
                face_order[0],
                near_tiles[0, 0],
                basis_right[0, 0],
                rank_scale,
                rank_counts,
                coupling[0],
                basis_left[0, 0],
            )
        ]
    )
    return out[None, None]


def solution(mesh):
    placed = (
        P("sub", "grp", None, None),
        P("sub", "grp", None, None),
        P("sub", "grp", None),
        P("sub", "grp", None, None, None),
        P("sub", "grp", None, None),
        P("sub", None),
        P(),
        P("sub", None, None, None),
        P("sub", "grp", None, None),
    )
    two = mesh.shape["sub"] == 2 * QUARTERS
    body = functools.partial(two_layers, mesh.shape["grp"]) if two else per_device
    return jax.shard_map(
        body,
        mesh=mesh,
        in_specs=placed,
        out_specs=P("sub", "grp", None, None),
        check_vma=False,
    )
```

```python
import functools
import jax
import jax.numpy as jnp
from jax import lax
from jax.experimental import pallas as pl
from jax.experimental.pallas import tpu as pltpu
from jax.sharding import PartitionSpec as P

FACE_Q = 192
ITERS = 3


def from_partner(value, axis, distance):
    mask = 2**distance
    pairs = [(source, source ^ mask) for source in range(lax.axis_size(axis))]
    return lax.ppermute(value, axis, pairs)


def shifted(value, axis, steps):
    count = lax.axis_size(axis)
    first, last = (max(0, -steps), min(count, count - steps))
    return lax.ppermute(value, axis, [(source, source + steps) for source in range(first, last)])


def per_device(
    impedance,
    incident,
    face_order,
    near_tiles,
    basis_right,
    rank_scale,
    rank_counts,
    coupling,
    basis_left,
):
    z_cols = impedance[0, 0]
    source = incident[0, 0]
    order_map = face_order[0, 0]
    tiles = near_tiles[0, 0]
    right_basis = basis_right[0, 0]
    left_basis = basis_left[0, 0]
    couple_rows = coupling[0]
    position = lax.axis_index("sub")
    cluster = position // 4
    rank_ids = jnp.arange(rank_scale.shape[1])
    kept = jnp.where(rank_ids < rank_counts[cluster], rank_scale[0], jnp.float32(0.0))
    trace_now = source
    for sweep_index in range(ITERS):
        whole = trace_now
        for bit_number in (0, 1):
            partner = from_partner(whole, "sub", bit_number)
            upper_half = position // (1 << bit_number) % 2 == 1
            whole = jnp.where(
                upper_half,
                jnp.concatenate([partner, whole], 1),
                jnp.concatenate([whole, partner], 1),
            )
        outgoing = jnp.dot(whole, z_cols, preferred_element_type=jnp.float32).astype(jnp.bfloat16)
        lower_out = outgoing[:, :FACE_Q]
        upper_out = outgoing[:, FACE_Q : 2 * FACE_Q]
        outer_out = outgoing[:, 2 * FACE_Q :]
        partial_sum = jnp.dot(outer_out, right_basis, preferred_element_type=jnp.float32)
        total = lax.psum(partial_sum.astype(jnp.bfloat16), "grp").astype(jnp.float32)
        coefs = (total * kept).astype(jnp.bfloat16)
        block_rows = lax.all_gather(coefs[None], "sub", axis=0, tiled=True)
        sources = jnp.arange(block_rows.shape[0]) // 4
        chosen = jnp.take(couple_rows, sources, axis=0)
        chosen = jnp.where((sources != cluster)[:, None, None], chosen, jnp.zeros_like(chosen))
        far = jnp.einsum(
            "nkr,nrt->kt", block_rows, chosen, preferred_element_type=jnp.float32
        ).astype(jnp.bfloat16)
        arrived = []
        for offset in (4, -4):
            sent = (upper_out, outer_out) if offset > 0 else (lower_out, outer_out)
            arrived.append(shifted((sent[0], sent[1]), "sub", offset))
        upper_below, outer_below = arrived[0]
        lower_above, outer_above = arrived[1]
        lower_in = jnp.take(upper_below, order_map, axis=1)
        outer_in = jnp.dot(outer_out, tiles[0], preferred_element_type=jnp.float32)
        outer_in = outer_in + jnp.dot(outer_below, tiles[1], preferred_element_type=jnp.float32)
        outer_in = outer_in + jnp.dot(outer_above, tiles[2], preferred_element_type=jnp.float32)
        outer_in = outer_in + jnp.dot(far, left_basis, preferred_element_type=jnp.float32)
        joined = jnp.concatenate(
            [lower_in.astype(jnp.float32), lower_above.astype(jnp.float32), outer_in], 1
        )
        trace_now = (joined + source.astype(jnp.float32)).astype(jnp.bfloat16)
    return trace_now[None, None]


QUARTERS = 4
F32 = jnp.float32
BF16 = jnp.bfloat16


def dot(a, b):
    return jnp.dot(a, b, preferred_element_type=F32)


def two_layer_kernel(
    groups,
    z_hbm,
    inc_hbm,
    order_hbm,
    tiles_hbm,
    right_hbm,
    scale_hbm,
    counts_hbm,
    couple_hbm,
    left_hbm,
    out_ref,
    own_ref,
    cross_ref,
    cross_there,
    right_ref,
    scale_ref,
    counts_ref,
    couple_ref,
    left_ref,
    z_ref,
    inc_all,
    order_all,
    left_all,
    all_w,
    g_all,
    base,
    mine,
    sourced,
    owned,
    other,
    plane_sum,
    other_sum,
    z_sem,
    load_sem,
    const_send,
    const_recv,
    send,
    recv,
    far_send,
    far_recv,
    g_send,
    g_recv,
    cross_send,
    cross_recv,
    slab_sem,
    ready_sem,
    go_sem,
):
    sub = lax.axis_index("sub")
    grp = lax.axis_index("grp")
    layer = sub // QUARTERS
    q = sub % QUARTERS
    exc, width = inc_all.shape[1:]
    half = exc // 2
    rank = right_ref.shape[1]
    outer = own_ref.shape[1]
    face = order_all.shape[2]
    upper = layer == 1
    flip0 = sub + 1 - 2 * (sub % 2)
    flip1 = sub + 2 - 4 * ((sub // 2) % 2)
    flip01 = flip1 + 1 - 2 * (flip1 % 2)
    flip2 = sub + 4 - 8 * layer
    flip12 = flip1 + 4 - 8 * layer
    q1 = flip0 % QUARTERS
    q2 = flip1 % QUARTERS
    q3 = flip01 % QUARTERS

    def remote(src, dst, send_sem, recv_sem, to_sub, to_grp=None):
        return pltpu.make_async_remote_copy(
            src_ref=src,
            dst_ref=dst,
            send_sem=send_sem,
            recv_sem=recv_sem,
            device_id=(to_sub, grp if to_grp is None else to_grp),
            device_id_type=pl.DeviceIdType.MESH,
        )

    def signal(sem, to_sub, to_grp):
        pl.semaphore_signal(
            sem, inc=1, device_id=(to_sub, to_grp), device_id_type=pl.DeviceIdType.MESH
        )

    loads = {}
    for i, (name, src, dst) in enumerate(
        [
            ("inc", inc_hbm, inc_all.at[q]),
            ("right", right_hbm, right_ref),
            ("scale", scale_hbm, scale_ref),
            ("counts", counts_hbm, counts_ref),
            ("couple", couple_hbm, couple_ref),
            ("left", left_hbm, left_ref),
            ("own", tiles_hbm.at[0], own_ref),
            ("cross", tiles_hbm.at[2 - layer], cross_ref),
            ("order", order_hbm, order_all.at[q]),
        ]
    ):
        loads[name] = pltpu.make_async_copy(src, dst, load_sem.at[i])
        loads[name].start()
    z_copies = []
    for part in range(QUARTERS):
        rows = pl.ds(part * width, width)
        copy = pltpu.make_async_copy(z_hbm.at[rows], z_ref.at[rows], z_sem.at[part])
        copy.start()
        z_copies.append(copy)

    slab = 2 * QUARTERS
    lead = sub == 0
    barrier = pltpu.get_barrier_semaphore()

    @pl.when(lead)
    def _():
        for i in range(1, slab):
            signal(barrier, i, grp)
        for d in range(1, groups):
            signal(barrier, sub, lax.rem(grp + d, groups))

    @pl.when(jnp.logical_not(lead))
    def _():
        for i in range(1, slab - 1):
            signal(barrier, 1 + lax.rem(sub - 1 + i, slab - 1), grp)
        pl.semaphore_wait(barrier, slab - 1)
        signal(slab_sem, 0, grp)

    @pl.when(lead)
    def _():
        pl.semaphore_wait(slab_sem, slab - 1)

    pending = []
    buffers = [inc_all, left_all, order_all]
    firsts = {}

    def const_start(i):
        buf = buffers[i]
        a = remote(buf.at[q], buf.at[q], const_send.at[i, 0], const_recv.at[i, 0], flip1)
        b = remote(buf.at[q], buf.at[q], const_send.at[i, 1], const_recv.at[i, 1], flip0)
        a.start()
        b.start()
        firsts[i] = (a, b)
        pending.extend([a, b])

    def const_forward(i):
        buf = buffers[i]
        firsts[i][0].wait_recv()
        c = remote(buf.at[q2], buf.at[q2], const_send.at[i, 2], const_recv.at[i, 2], flip0)
        c.start()
        pending.append(c)
        return c

    loads["inc"].wait()
    const_start(0)

    loads["cross"].wait()
    cross_copy = remote(cross_ref, cross_there, cross_send, cross_recv, flip2)
    cross_copy.start()
    pending.append(cross_copy)
    for name in ("right", "scale", "counts", "couple", "left", "own", "order"):
        loads[name].wait()
    lanes = lax.broadcasted_iota(jnp.int32, (1, rank), 1)
    kept = jnp.where(lanes < counts_ref[layer], scale_ref[...], F32(0.0))
    right_ref[...] = (right_ref[...].astype(F32) * kept).astype(BF16)
    left_all[q] = dot(couple_ref[1 - layer], left_ref[...]).astype(BF16)

    @pl.when(lead)
    def _():
        pl.semaphore_wait(barrier, groups - 1)
        for d in range(1, groups):
            signal(ready_sem, sub, lax.rem(grp + d, groups))

    for copy in z_copies:
        copy.wait()

    def z_quarter(index):
        return z_ref[pl.ds(pl.multiple_of(index * width, width), width), :]

    acc = dot(inc_all[q], z_quarter(q))
    firsts[0][1].wait_recv()
    acc = acc + dot(inc_all[q1], z_quarter(q1))
    for i in (1, 2):
        const_start(i)

    @pl.when(lead)
    def _():
        pl.semaphore_wait(ready_sem, groups - 1)
        for i in range(1, slab):
            signal(go_sem, i, grp)

    fwd = const_forward(0)
    acc = acc + dot(inc_all[q2], z_quarter(q2))
    fwd.wait_recv()
    acc = acc + dot(inc_all[q3], z_quarter(q3))
    base[...] = acc

    lane = lax.broadcasted_iota(jnp.int32, (half, outer), 1)
    low = lane < outer // 2
    first_here = low == upper
    first_there = low != upper
    slot = lax.broadcasted_iota(jnp.int32, (2 * outer, 2 * face), 0)
    in_half = slot % (outer // 2)
    full_entry = jnp.where(upper, slot + outer // 2, slot)
    half_entry = jnp.where(upper, in_half, in_half + outer)
    entry = jnp.where(slot < outer, full_entry, half_entry)
    along = lax.broadcasted_iota(jnp.int32, (1, face), 1)
    nothing = jnp.full((1, face), -1, jnp.int32)
    far_at = 3 * QUARTERS * outer

    def chosen(order_row):
        below = jnp.where(upper, order_row, nothing)
        above = jnp.where(upper, nothing, along)
        wanted = jnp.concatenate([below, above], 1)
        return jnp.where(entry == wanted, F32(1.0), F32(0.0)).astype(BF16)

    def face_tiles(block):
        full = block[exc : 2 * exc]
        packed = block[2 * exc : 2 * exc + half]
        zero = jnp.zeros_like(packed)
        top = jnp.where(first_there, packed, zero)
        bottom = jnp.where(first_there, zero, packed)
        return jnp.concatenate([full, jnp.concatenate([top, bottom], 0)], 1)

    def weights():
        for part in range(QUARTERS):
            start, at = part * width, 3 * part * outer
            z_outer = z_ref[start + 2 * face : start + width, :]
            all_w[at : at + outer, :] = z_outer
            term = dot(left_all[part], z_outer)
            total = term if part == 0 else total + term
            z_face = z_ref[start : start + 2 * face, :]
            all_w[at + outer : at + 3 * outer, :] = dot(chosen(order_all[part]), z_face).astype(BF16)
        all_w[far_at : far_at + rank, :] = total.astype(BF16)

    def to_plane(buf, sweep, first_sem, value):
        buf[sweep, q] = value.astype(BF16)
        at = buf.at[sweep, q]
        copies = []
        for sem, peer in ((first_sem, flip01), (first_sem + 1, flip1), (first_sem + 2, flip0)):
            copy = remote(at, at, send.at[sweep, sem], recv.at[sweep, sem], peer)
            copy.start()
            copies.append(copy)
            pending.append(copy)
        return copies[::-1]

    def start_source(sweep, outer_out):
        return to_plane(sourced, sweep, 2, dot(outer_out, right_ref[...]))

    def start_own(sweep, outer_out):
        owned[sweep, q] = dot(outer_out, own_ref[...]).astype(BF16)
        at = owned.at[sweep, q]
        ss, rs = send.at[sweep], recv.at[sweep]
        v_x = remote(at, at, ss.at[8], rs.at[8], flip1)
        v_c = remote(at, at, ss.at[9], rs.at[9], flip0)
        v_x.start()
        v_c.start()
        pending.extend([v_x, v_c])
        return v_c, v_x

    def forward_own(sweep, own):
        own[1].wait_recv()
        at = owned.at[sweep, q2]
        v_f = remote(at, at, send.at[sweep, 7], recv.at[sweep, 7], flip0)
        v_f.start()
        pending.append(v_f)
        return v_f

    def start_near(sweep, acc):
        ss, rs = send.at[sweep], recv.at[sweep]
        mid = acc[:, outer : 2 * outer]
        rolled = pltpu.roll(mid, outer // 2, 1)
        crossed = dot(acc[:, 2 * face :].astype(BF16), cross_there[...])
        mine[sweep, 0:exc] = crossed.astype(BF16)
        mine[sweep, exc : 2 * exc] = jnp.where(upper, acc[:, 0:outer], acc[:, 2 * outer : 3 * outer]).astype(BF16)
        mine[sweep, 2 * exc : 2 * exc + half] = jnp.where(first_here, mid[:half], rolled[half:]).astype(BF16)
        w_y = remote(mine.at[sweep], other.at[sweep, q], ss.at[0], rs.at[0], flip2)
        copies = [w_y]
        if sweep < ITERS - 1:
            copies.append(remote(mine.at[sweep], other.at[sweep, q], ss.at[1], rs.at[1], flip12))
        for copy in copies:
            copy.start()
            pending.append(copy)
        return copies

    def start_sums(sweep, value):
        plane_sum[sweep] = value.astype(BF16)
        sums = []
        for d in sorted(range(groups), key=lambda d: -min(d, groups - d)):
            copy = remote(
                plane_sum.at[sweep],
                other_sum.at[sweep, d],
                far_send.at[sweep, d],
                far_recv.at[sweep, d],
                flip2,
                lax.rem(grp + d, groups),
            )
            copy.start()
            sums.append(copy)
            pending.append(copy)
        return sums

    def far_total(sweep, sums):
        for copy in sums:
            copy.wait_recv()
        total = other_sum[sweep, 0].astype(F32)
        for d in range(1, groups):
            total = total + other_sum[sweep, d].astype(F32)
        return total.astype(BF16)

    def near_block(sweep, part):
        block = other[sweep, part]
        outer_in = owned[sweep, part].astype(F32) + block[:exc].astype(F32)
        return jnp.concatenate([outer_in.astype(BF16), face_tiles(block)], 1)

    def near_rows(part):
        at = pl.multiple_of(3 * part * outer, outer)
        return all_w[pl.ds(at, 3 * outer), :]

    def known_terms(sweep, near, own):
        w_y, w_d = near
        ss, rs = send.at[sweep], recv.at[sweep]
        y_f = remote(other.at[sweep, q], other.at[sweep, q], ss.at[5], rs.at[5], flip0)
        d_f = remote(other.at[sweep, q2], other.at[sweep, q2], ss.at[6], rs.at[6], flip0)
        pending.extend([y_f, d_f])
        w_y.wait_recv()
        y_f.start()
        v_f = forward_own(sweep, own)
        known = base[...] + dot(near_block(sweep, q), near_rows(q))
        w_d.wait_recv()
        d_f.start()
        known = known + dot(near_block(sweep, q2), near_rows(q2))
        own[0].wait_recv()
        y_f.wait_recv()
        known = known + dot(near_block(sweep, q1), near_rows(q1))
        v_f.wait_recv()
        d_f.wait_recv()
        block, rows = near_block(sweep, q3), near_rows(q3)
        known_outer = known[:, 2 * face :] + dot(block, rows[:, 2 * face :])
        ahead = None
        if sweep == ITERS - 2:
            ahead = start_source(sweep + 1, known_outer.astype(BF16))
        known_face = known[:, : 2 * face] + dot(block, rows[:, : 2 * face])
        return jnp.concatenate([known_face, known_outer], 1), ahead

    for sweep in range(ITERS):
        last = sweep == ITERS - 1
        outer_out = acc[:, 2 * face :].astype(BF16)
        if sweep == 0:
            outs = start_source(sweep, outer_out)
            cross_copy.wait_recv()
            near = start_near(sweep, acc)
            own = start_own(sweep, outer_out)
            consts = [const_forward(1), const_forward(2)]
        elif not last:
            near = start_near(sweep, acc)
            outs = start_source(sweep, outer_out)
            own = start_own(sweep, outer_out)
        else:
            near = start_near(sweep, acc)
            outs = ahead
        if last:
            for copy in shares:
                copy.wait_recv()
            whole = g_all[0].astype(F32)
            for part in range(1, QUARTERS):
                whole = whole + g_all[part].astype(F32)
            value = dot(total, whole.astype(BF16))
        for copy in outs:
            copy.wait_recv()
        for part in range(QUARTERS):
            term = sourced[sweep, part].astype(F32)
            value = value + term if last or part else term
        if sweep == 0:

            @pl.when(jnp.logical_not(lead))
            def _():
                pl.semaphore_wait(go_sem, 1)

        sums = start_sums(sweep, value)
        if sweep == 0:
            for i in (1, 2):
                firsts[i][1].wait_recv()
            for c in consts:
                c.wait_recv()
            weights()
            far_outer = all_w[far_at : far_at + rank, 2 * face :]
            g_all[q] = dot(far_outer, right_ref[...]).astype(BF16)
            shares = [
                remote(g_all.at[q], g_all.at[q], g_send.at[i], g_recv.at[i], peer)
                for i, peer in enumerate((flip01, flip1, flip0))
            ]
            for copy in shares:
                copy.start()
                pending.append(copy)
        if not last:
            known, ahead = known_terms(sweep, near, own)
            total = far_total(sweep, sums)
            acc = known + dot(total, all_w[far_at : far_at + rank, :])
        else:
            near[0].wait_recv()
            block = other[sweep, q]
            outer_in = dot(outer_out, own_ref[...]) + block[:exc].astype(F32)
            faces = dot(face_tiles(block), chosen(order_all[q]))
            inc = inc_all[q].astype(F32)
            out_ref[:, 0 : 2 * face] = (faces + inc[:, : 2 * face]).astype(BF16)
            outer_in = outer_in + inc[:, 2 * face :]
            total = far_total(sweep, sums)
            outer_in = outer_in + dot(total, left_all[q])
            out_ref[:, 2 * face :] = outer_in.astype(BF16)
    for copy in pending:
        copy.wait_send()


def two_layers(
    groups,
    impedance,
    incident,
    face_order,
    near_tiles,
    basis_right,
    rank_scale,
    rank_counts,
    coupling,
    basis_left,
):
    order, width = impedance.shape[2:]
    exc = incident.shape[2]
    face = face_order.shape[2]
    outer = near_tiles.shape[3]
    rank = basis_right.shape[3]
    vmem = pl.BlockSpec(memory_space=pltpu.VMEM)
    dma = pltpu.SemaphoreType.DMA
    block = 2 * exc + exc // 2
    out = pl.pallas_call(
        functools.partial(two_layer_kernel, groups),
        out_shape=jax.ShapeDtypeStruct((exc, width), BF16),
        in_specs=[pl.BlockSpec(memory_space=pltpu.HBM)] * 9,
        out_specs=vmem,
        scratch_shapes=[
            pltpu.VMEM((outer, outer), BF16),
            pltpu.VMEM((outer, outer), BF16),
            pltpu.VMEM((outer, outer), BF16),
            pltpu.VMEM((outer, rank), BF16),
            pltpu.VMEM((1, rank), F32),
            pltpu.SMEM(rank_counts.shape, jnp.int32),
            pltpu.VMEM(coupling.shape[1:], BF16),
            pltpu.VMEM((rank, outer), BF16),
            pltpu.VMEM((order, width), BF16),
            pltpu.VMEM((QUARTERS, exc, width), BF16),
            pltpu.VMEM((QUARTERS, 1, face), jnp.int32),
            pltpu.VMEM((QUARTERS, rank, outer), BF16),
            pltpu.VMEM((3 * QUARTERS * outer + rank, width), BF16),
            pltpu.VMEM((QUARTERS, rank, rank), BF16),
            pltpu.VMEM((exc, width), F32),
            pltpu.VMEM((ITERS, block, outer), BF16),
            pltpu.VMEM((ITERS, QUARTERS, exc, rank), BF16),
            pltpu.VMEM((ITERS, QUARTERS, exc, outer), BF16),
            pltpu.VMEM((ITERS, QUARTERS, block, outer), BF16),
            pltpu.VMEM((ITERS, exc, rank), BF16),
            pltpu.VMEM((ITERS, groups, exc, rank), BF16),
            dma((QUARTERS,)),
            dma((9,)),
            dma((3, 3)),
            dma((3, 3)),
            dma((ITERS, 10)),
            dma((ITERS, 10)),
            dma((ITERS, groups)),
            dma((ITERS, groups)),
            dma((3,)),
            dma((3,)),
            dma,
            dma,
            pltpu.SemaphoreType.REGULAR,
            pltpu.SemaphoreType.REGULAR,
            pltpu.SemaphoreType.REGULAR,
        ],
        compiler_params=pltpu.CompilerParams(
            collective_id=0, has_side_effects=True, vmem_limit_bytes=48 * 1024 * 1024
        ),
    )(
        *[
            pltpu.with_memory_space_constraint(operand, pltpu.HBM)
            for operand in (
                impedance[0, 0],
                incident[0, 0],
                face_order[0],
                near_tiles[0, 0],
                basis_right[0, 0],
                rank_scale,
                rank_counts,
                coupling[0],
                basis_left[0, 0],
            )
        ]
    )
    return out[None, None]


def solution(mesh):
    placed = (
        P("sub", "grp", None, None),
        P("sub", "grp", None, None),
        P("sub", "grp", None),
        P("sub", "grp", None, None, None),
        P("sub", "grp", None, None),
        P("sub", None),
        P(),
        P("sub", None, None, None),
        P("sub", "grp", None, None),
    )
    two = mesh.shape["sub"] == 2 * QUARTERS
    body = functools.partial(two_layers, mesh.shape["grp"]) if two else per_device
    return jax.shard_map(
        body,
        mesh=mesh,
        in_specs=placed,
        out_specs=P("sub", "grp", None, None),
        check_vma=False,
    )
```

```python
import functools
import jax
import jax.numpy as jnp
from jax import lax
from jax.experimental import pallas as pl
from jax.experimental.pallas import tpu as pltpu
from jax.sharding import PartitionSpec as P

FACE_Q = 192
ITERS = 3


def from_partner(value, axis, distance):
    mask = 2**distance
    pairs = [(source, source ^ mask) for source in range(lax.axis_size(axis))]
    return lax.ppermute(value, axis, pairs)


def shifted(value, axis, steps):
    count = lax.axis_size(axis)
    first, last = (max(0, -steps), min(count, count - steps))
    return lax.ppermute(value, axis, [(source, source + steps) for source in range(first, last)])


def per_device(
    impedance,
    incident,
    face_order,
    near_tiles,
    basis_right,
    rank_scale,
    rank_counts,
    coupling,
    basis_left,
):
    z_cols = impedance[0, 0]
    source = incident[0, 0]
    order_map = face_order[0, 0]
    tiles = near_tiles[0, 0]
    right_basis = basis_right[0, 0]
    left_basis = basis_left[0, 0]
    couple_rows = coupling[0]
    position = lax.axis_index("sub")
    cluster = position // 4
    rank_ids = jnp.arange(rank_scale.shape[1])
    kept = jnp.where(rank_ids < rank_counts[cluster], rank_scale[0], jnp.float32(0.0))
    trace_now = source
    for sweep_index in range(ITERS):
        whole = trace_now
        for bit_number in (0, 1):
            partner = from_partner(whole, "sub", bit_number)
            upper_half = position // (1 << bit_number) % 2 == 1
            whole = jnp.where(
                upper_half,
                jnp.concatenate([partner, whole], 1),
                jnp.concatenate([whole, partner], 1),
            )
        outgoing = jnp.dot(whole, z_cols, preferred_element_type=jnp.float32).astype(jnp.bfloat16)
        lower_out = outgoing[:, :FACE_Q]
        upper_out = outgoing[:, FACE_Q : 2 * FACE_Q]
        outer_out = outgoing[:, 2 * FACE_Q :]
        partial_sum = jnp.dot(outer_out, right_basis, preferred_element_type=jnp.float32)
        total = lax.psum(partial_sum.astype(jnp.bfloat16), "grp").astype(jnp.float32)
        coefs = (total * kept).astype(jnp.bfloat16)
        block_rows = lax.all_gather(coefs[None], "sub", axis=0, tiled=True)
        sources = jnp.arange(block_rows.shape[0]) // 4
        chosen = jnp.take(couple_rows, sources, axis=0)
        chosen = jnp.where((sources != cluster)[:, None, None], chosen, jnp.zeros_like(chosen))
        far = jnp.einsum(
            "nkr,nrt->kt", block_rows, chosen, preferred_element_type=jnp.float32
        ).astype(jnp.bfloat16)
        arrived = []
        for offset in (4, -4):
            sent = (upper_out, outer_out) if offset > 0 else (lower_out, outer_out)
            arrived.append(shifted((sent[0], sent[1]), "sub", offset))
        upper_below, outer_below = arrived[0]
        lower_above, outer_above = arrived[1]
        lower_in = jnp.take(upper_below, order_map, axis=1)
        outer_in = jnp.dot(outer_out, tiles[0], preferred_element_type=jnp.float32)
        outer_in = outer_in + jnp.dot(outer_below, tiles[1], preferred_element_type=jnp.float32)
        outer_in = outer_in + jnp.dot(outer_above, tiles[2], preferred_element_type=jnp.float32)
        outer_in = outer_in + jnp.dot(far, left_basis, preferred_element_type=jnp.float32)
        joined = jnp.concatenate(
            [lower_in.astype(jnp.float32), lower_above.astype(jnp.float32), outer_in], 1
        )
        trace_now = (joined + source.astype(jnp.float32)).astype(jnp.bfloat16)
    return trace_now[None, None]


QUARTERS = 4
F32 = jnp.float32
BF16 = jnp.bfloat16


def dot(a, b):
    return jnp.dot(a, b, preferred_element_type=F32)


def two_layer_kernel(
    groups,
    z_hbm,
    inc_hbm,
    order_hbm,
    tiles_hbm,
    right_hbm,
    scale_hbm,
    counts_hbm,
    couple_hbm,
    left_hbm,
    out_ref,
    own_ref,
    cross_ref,
    cross_there,
    right_ref,
    scale_ref,
    counts_ref,
    couple_ref,
    left_ref,
    z_ref,
    inc_all,
    order_all,
    left_all,
    all_w,
    g_all,
    base,
    mine,
    sourced,
    owned,
    other,
    plane_sum,
    other_sum,
    z_sem,
    load_sem,
    const_send,
    const_recv,
    send,
    recv,
    far_send,
    far_recv,
    g_send,
    g_recv,
    cross_send,
    cross_recv,
    slab_sem,
    ready_sem,
    go_sem,
):
    sub = lax.axis_index("sub")
    grp = lax.axis_index("grp")
    layer = sub // QUARTERS
    q = sub % QUARTERS
    exc, width = inc_all.shape[1:]
    half = exc // 2
    rank = right_ref.shape[1]
    outer = own_ref.shape[1]
    face = order_all.shape[2]
    upper = layer == 1
    flip0 = sub + 1 - 2 * (sub % 2)
    flip1 = sub + 2 - 4 * ((sub // 2) % 2)
    flip01 = flip1 + 1 - 2 * (flip1 % 2)
    flip2 = sub + 4 - 8 * layer
    flip12 = flip1 + 4 - 8 * layer
    q1 = flip0 % QUARTERS
    q2 = flip1 % QUARTERS
    q3 = flip01 % QUARTERS

    def remote(src, dst, send_sem, recv_sem, to_sub, to_grp=None):
        return pltpu.make_async_remote_copy(
            src_ref=src,
            dst_ref=dst,
            send_sem=send_sem,
            recv_sem=recv_sem,
            device_id=(to_sub, grp if to_grp is None else to_grp),
            device_id_type=pl.DeviceIdType.MESH,
        )

    def signal(sem, to_sub, to_grp):
        pl.semaphore_signal(
            sem, inc=1, device_id=(to_sub, to_grp), device_id_type=pl.DeviceIdType.MESH
        )

    loads = {}
    for i, (name, src, dst) in enumerate(
        [
            ("inc", inc_hbm, inc_all.at[q]),
            ("right", right_hbm, right_ref),
            ("scale", scale_hbm, scale_ref),
            ("counts", counts_hbm, counts_ref),
            ("couple", couple_hbm, couple_ref),
            ("left", left_hbm, left_ref),
            ("own", tiles_hbm.at[0], own_ref),
            ("cross", tiles_hbm.at[2 - layer], cross_ref),
            ("order", order_hbm, order_all.at[q]),
        ]
    ):
        loads[name] = pltpu.make_async_copy(src, dst, load_sem.at[i])
        loads[name].start()
    z_copies = []
    for part in range(QUARTERS):
        rows = pl.ds(part * width, width)
        copy = pltpu.make_async_copy(z_hbm.at[rows], z_ref.at[rows], z_sem.at[part])
        copy.start()
        z_copies.append(copy)

    slab = 2 * QUARTERS
    lead = sub == 0
    barrier = pltpu.get_barrier_semaphore()

    @pl.when(lead)
    def _():
        for i in range(1, slab):
            signal(barrier, i, grp)
        for d in range(1, groups):
            signal(barrier, sub, lax.rem(grp + d, groups))

    @pl.when(jnp.logical_not(lead))
    def _():
        for i in range(1, slab - 1):
            signal(barrier, 1 + lax.rem(sub - 1 + i, slab - 1), grp)
        pl.semaphore_wait(barrier, slab - 1)
        signal(slab_sem, 0, grp)

    @pl.when(lead)
    def _():
        pl.semaphore_wait(slab_sem, slab - 1)

    pending = []
    buffers = [inc_all, left_all, order_all]
    firsts = {}

    def const_start(i):
        buf = buffers[i]
        a = remote(buf.at[q], buf.at[q], const_send.at[i, 0], const_recv.at[i, 0], flip1)
        b = remote(buf.at[q], buf.at[q], const_send.at[i, 1], const_recv.at[i, 1], flip0)
        a.start()
        b.start()
        firsts[i] = (a, b)
        pending.extend([a, b])

    def const_forward(i):
        buf = buffers[i]
        firsts[i][0].wait_recv()
        c = remote(buf.at[q2], buf.at[q2], const_send.at[i, 2], const_recv.at[i, 2], flip0)
        c.start()
        pending.append(c)
        return c

    loads["inc"].wait()
    cut = exc * 1 // 2 // 16 * 16
    head = inc_all.at[q, pl.ds(0, cut)]
    tail = inc_all.at[q, pl.ds(cut, exc - cut)]
    inc_x = remote(head, head, const_send.at[0, 0], const_recv.at[0, 0], flip1)
    inc_c = remote(inc_all.at[q], inc_all.at[q], const_send.at[0, 1], const_recv.at[0, 1], flip0)
    inc_tx = remote(tail, tail, const_send.at[3, 0], const_recv.at[3, 0], flip1)
    inc_td = remote(tail, tail, const_send.at[3, 1], const_recv.at[3, 1], flip01)
    for copy in (inc_x, inc_c, inc_td, inc_tx):
        copy.start()
        pending.append(copy)

    loads["cross"].wait()
    cross_copy = remote(cross_ref, cross_there, cross_send, cross_recv, flip2)
    cross_copy.start()
    pending.append(cross_copy)
    for name in ("right", "scale", "counts", "couple", "left", "own", "order"):
        loads[name].wait()
    lanes = lax.broadcasted_iota(jnp.int32, (1, rank), 1)
    kept = jnp.where(lanes < counts_ref[layer], scale_ref[...], F32(0.0))
    right_ref[...] = (right_ref[...].astype(F32) * kept).astype(BF16)
    left_all[q] = dot(couple_ref[1 - layer], left_ref[...]).astype(BF16)

    @pl.when(lead)
    def _():
        pl.semaphore_wait(barrier, groups - 1)
        for d in range(1, groups):
            signal(ready_sem, sub, lax.rem(grp + d, groups))

    for copy in z_copies:
        copy.wait()

    def z_quarter(index):
        return z_ref[pl.ds(pl.multiple_of(index * width, width), width), :]

    acc = dot(inc_all[q], z_quarter(q))
    inc_c.wait_recv()
    acc = acc + dot(inc_all[q1], z_quarter(q1))
    for i in (1, 2):
        const_start(i)

    @pl.when(lead)
    def _():
        pl.semaphore_wait(ready_sem, groups - 1)
        for i in range(1, slab):
            signal(go_sem, i, grp)

    inc_x.wait_recv()
    moved = inc_all.at[q2, pl.ds(0, cut)]
    fwd = remote(moved, moved, const_send.at[0, 2], const_recv.at[0, 2], flip0)
    fwd.start()
    pending.append(fwd)
    inc_tx.wait_recv()
    acc = acc + dot(inc_all[q2], z_quarter(q2))
    inc_td.wait_recv()
    fwd.wait_recv()
    acc = acc + dot(inc_all[q3], z_quarter(q3))
    base[...] = acc

    lane = lax.broadcasted_iota(jnp.int32, (half, outer), 1)
    low = lane < outer // 2
    first_here = low == upper
    first_there = low != upper
    slot = lax.broadcasted_iota(jnp.int32, (2 * outer, 2 * face), 0)
    in_half = slot % (outer // 2)
    full_entry = jnp.where(upper, slot + outer // 2, slot)
    half_entry = jnp.where(upper, in_half, in_half + outer)
    entry = jnp.where(slot < outer, full_entry, half_entry)
    along = lax.broadcasted_iota(jnp.int32, (1, face), 1)
    nothing = jnp.full((1, face), -1, jnp.int32)
    far_at = 3 * QUARTERS * outer

    def chosen(order_row):
        below = jnp.where(upper, order_row, nothing)
        above = jnp.where(upper, nothing, along)
        wanted = jnp.concatenate([below, above], 1)
        return jnp.where(entry == wanted, F32(1.0), F32(0.0)).astype(BF16)

    def face_tiles(block):
        full = block[exc : 2 * exc]
        packed = block[2 * exc : 2 * exc + half]
        zero = jnp.zeros_like(packed)
        top = jnp.where(first_there, packed, zero)
        bottom = jnp.where(first_there, zero, packed)
        return jnp.concatenate([full, jnp.concatenate([top, bottom], 0)], 1)

    def weights():
        for part in range(QUARTERS):
            start, at = part * width, 3 * part * outer
            z_outer = z_ref[start + 2 * face : start + width, :]
            all_w[at : at + outer, :] = z_outer
            term = dot(left_all[part], z_outer)
            total = term if part == 0 else total + term
            z_face = z_ref[start : start + 2 * face, :]
            all_w[at + outer : at + 3 * outer, :] = dot(chosen(order_all[part]), z_face).astype(BF16)
        all_w[far_at : far_at + rank, :] = total.astype(BF16)

    def to_plane(buf, sweep, first_sem, value):
        buf[sweep, q] = value.astype(BF16)
        at = buf.at[sweep, q]
        copies = []
        for sem, peer in ((first_sem, flip01), (first_sem + 1, flip1), (first_sem + 2, flip0)):
            copy = remote(at, at, send.at[sweep, sem], recv.at[sweep, sem], peer)
            copy.start()
            copies.append(copy)
            pending.append(copy)
        return copies[::-1]

    def start_source(sweep, outer_out):
        return to_plane(sourced, sweep, 2, dot(outer_out, right_ref[...]))

    def start_own(sweep, outer_out):
        owned[sweep, q] = dot(outer_out, own_ref[...]).astype(BF16)
        at = owned.at[sweep, q]
        ss, rs = send.at[sweep], recv.at[sweep]
        v_x = remote(at, at, ss.at[8], rs.at[8], flip1)
        v_c = remote(at, at, ss.at[9], rs.at[9], flip0)
        v_x.start()
        v_c.start()
        pending.extend([v_x, v_c])
        return v_c, v_x

    def forward_own(sweep, own):
        own[1].wait_recv()
        at = owned.at[sweep, q2]
        v_f = remote(at, at, send.at[sweep, 7], recv.at[sweep, 7], flip0)
        v_f.start()
        pending.append(v_f)
        return v_f

    def start_near(sweep, acc):
        ss, rs = send.at[sweep], recv.at[sweep]
        mid = acc[:, outer : 2 * outer]
        rolled = pltpu.roll(mid, outer // 2, 1)
        crossed = dot(acc[:, 2 * face :].astype(BF16), cross_there[...])
        mine[sweep, 0:exc] = crossed.astype(BF16)
        mine[sweep, exc : 2 * exc] = jnp.where(upper, acc[:, 0:outer], acc[:, 2 * outer : 3 * outer]).astype(BF16)
        mine[sweep, 2 * exc : 2 * exc + half] = jnp.where(first_here, mid[:half], rolled[half:]).astype(BF16)
        w_y = remote(mine.at[sweep], other.at[sweep, q], ss.at[0], rs.at[0], flip2)
        copies = [w_y]
        if sweep < ITERS - 1:
            copies.append(remote(mine.at[sweep], other.at[sweep, q], ss.at[1], rs.at[1], flip12))
        for copy in copies:
            copy.start()
            pending.append(copy)
        return copies

    def start_sums(sweep, value):
        plane_sum[sweep] = value.astype(BF16)
        sums = []
        for d in sorted(range(groups), key=lambda d: -min(d, groups - d)):
            copy = remote(
                plane_sum.at[sweep],
                other_sum.at[sweep, d],
                far_send.at[sweep, d],
                far_recv.at[sweep, d],
                flip2,
                lax.rem(grp + d, groups),
            )
            copy.start()
            sums.append(copy)
            pending.append(copy)
        return sums

    def far_total(sweep, sums):
        for copy in sums:
            copy.wait_recv()
        total = other_sum[sweep, 0].astype(F32)
        for d in range(1, groups):
            total = total + other_sum[sweep, d].astype(F32)
        return total.astype(BF16)

    def near_block(sweep, part):
        block = other[sweep, part]
        outer_in = owned[sweep, part].astype(F32) + block[:exc].astype(F32)
        return jnp.concatenate([outer_in.astype(BF16), face_tiles(block)], 1)

    def near_rows(part):
        at = pl.multiple_of(3 * part * outer, outer)
        return all_w[pl.ds(at, 3 * outer), :]

    def known_terms(sweep, near, own):
        w_y, w_d = near
        ss, rs = send.at[sweep], recv.at[sweep]
        y_f = remote(other.at[sweep, q], other.at[sweep, q], ss.at[5], rs.at[5], flip0)
        d_f = remote(other.at[sweep, q2], other.at[sweep, q2], ss.at[6], rs.at[6], flip0)
        pending.extend([y_f, d_f])
        w_y.wait_recv()
        y_f.start()
        v_f = forward_own(sweep, own)
        known = base[...] + dot(near_block(sweep, q), near_rows(q))
        w_d.wait_recv()
        d_f.start()
        known = known + dot(near_block(sweep, q2), near_rows(q2))
        own[0].wait_recv()
        y_f.wait_recv()
        known = known + dot(near_block(sweep, q1), near_rows(q1))
        v_f.wait_recv()
        d_f.wait_recv()
        block, rows = near_block(sweep, q3), near_rows(q3)
        known_outer = known[:, 2 * face :] + dot(block, rows[:, 2 * face :])
        ahead = None
        if sweep == ITERS - 2:
            ahead = start_source(sweep + 1, known_outer.astype(BF16))
        known_face = known[:, : 2 * face] + dot(block, rows[:, : 2 * face])
        return jnp.concatenate([known_face, known_outer], 1), ahead

    for sweep in range(ITERS):
        last = sweep == ITERS - 1
        outer_out = acc[:, 2 * face :].astype(BF16)
        if sweep == 0:
            outs = start_source(sweep, outer_out)
            cross_copy.wait_recv()
            near = start_near(sweep, acc)
            own = start_own(sweep, outer_out)
            consts = [const_forward(1), const_forward(2)]
        elif not last:
            near = start_near(sweep, acc)
            outs = start_source(sweep, outer_out)
            own = start_own(sweep, outer_out)
        else:
            near = start_near(sweep, acc)
            outs = ahead
        if last:
            for copy in shares:
                copy.wait_recv()
            whole = g_all[0].astype(F32)
            for part in range(1, QUARTERS):
                whole = whole + g_all[part].astype(F32)
            value = dot(total, whole.astype(BF16))
        for copy in outs:
            copy.wait_recv()
        for part in range(QUARTERS):
            term = sourced[sweep, part].astype(F32)
            value = value + term if last or part else term
        if sweep == 0:

            @pl.when(jnp.logical_not(lead))
            def _():
                pl.semaphore_wait(go_sem, 1)

        sums = start_sums(sweep, value)
        if sweep == 0:
            for i in (1, 2):
                firsts[i][1].wait_recv()
            for c in consts:
                c.wait_recv()
            weights()
            far_outer = all_w[far_at : far_at + rank, 2 * face :]
            g_all[q] = dot(far_outer, right_ref[...]).astype(BF16)
            shares = [
                remote(g_all.at[q], g_all.at[q], g_send.at[i], g_recv.at[i], peer)
                for i, peer in enumerate((flip01, flip1, flip0))
            ]
            for copy in shares:
                copy.start()
                pending.append(copy)
        if not last:
            known, ahead = known_terms(sweep, near, own)
            total = far_total(sweep, sums)
            acc = known + dot(total, all_w[far_at : far_at + rank, :])
        else:
            near[0].wait_recv()
            block = other[sweep, q]
            outer_in = dot(outer_out, own_ref[...]) + block[:exc].astype(F32)
            faces = dot(face_tiles(block), chosen(order_all[q]))
            inc = inc_all[q].astype(F32)
            out_ref[:, 0 : 2 * face] = (faces + inc[:, : 2 * face]).astype(BF16)
            outer_in = outer_in + inc[:, 2 * face :]
            total = far_total(sweep, sums)
            outer_in = outer_in + dot(total, left_all[q])
            out_ref[:, 2 * face :] = outer_in.astype(BF16)
    for copy in pending:
        copy.wait_send()


def two_layers(
    groups,
    impedance,
    incident,
    face_order,
    near_tiles,
    basis_right,
    rank_scale,
    rank_counts,
    coupling,
    basis_left,
):
    order, width = impedance.shape[2:]
    exc = incident.shape[2]
    face = face_order.shape[2]
    outer = near_tiles.shape[3]
    rank = basis_right.shape[3]
    vmem = pl.BlockSpec(memory_space=pltpu.VMEM)
    dma = pltpu.SemaphoreType.DMA
    block = 2 * exc + exc // 2
    out = pl.pallas_call(
        functools.partial(two_layer_kernel, groups),
        out_shape=jax.ShapeDtypeStruct((exc, width), BF16),
        in_specs=[pl.BlockSpec(memory_space=pltpu.HBM)] * 9,
        out_specs=vmem,
        scratch_shapes=[
            pltpu.VMEM((outer, outer), BF16),
            pltpu.VMEM((outer, outer), BF16),
            pltpu.VMEM((outer, outer), BF16),
            pltpu.VMEM((outer, rank), BF16),
            pltpu.VMEM((1, rank), F32),
            pltpu.SMEM(rank_counts.shape, jnp.int32),
            pltpu.VMEM(coupling.shape[1:], BF16),
            pltpu.VMEM((rank, outer), BF16),
            pltpu.VMEM((order, width), BF16),
            pltpu.VMEM((QUARTERS, exc, width), BF16),
            pltpu.VMEM((QUARTERS, 1, face), jnp.int32),
            pltpu.VMEM((QUARTERS, rank, outer), BF16),
            pltpu.VMEM((3 * QUARTERS * outer + rank, width), BF16),
            pltpu.VMEM((QUARTERS, rank, rank), BF16),
            pltpu.VMEM((exc, width), F32),
            pltpu.VMEM((ITERS, block, outer), BF16),
            pltpu.VMEM((ITERS, QUARTERS, exc, rank), BF16),
            pltpu.VMEM((ITERS, QUARTERS, exc, outer), BF16),
            pltpu.VMEM((ITERS, QUARTERS, block, outer), BF16),
            pltpu.VMEM((ITERS, exc, rank), BF16),
            pltpu.VMEM((ITERS, groups, exc, rank), BF16),
            dma((QUARTERS,)),
            dma((9,)),
            dma((4, 3)),
            dma((4, 3)),
            dma((ITERS, 10)),
            dma((ITERS, 10)),
            dma((ITERS, groups)),
            dma((ITERS, groups)),
            dma((3,)),
            dma((3,)),
            dma,
            dma,
            pltpu.SemaphoreType.REGULAR,
            pltpu.SemaphoreType.REGULAR,
            pltpu.SemaphoreType.REGULAR,
        ],
        compiler_params=pltpu.CompilerParams(
            collective_id=0, has_side_effects=True, vmem_limit_bytes=48 * 1024 * 1024
        ),
    )(
        *[
            pltpu.with_memory_space_constraint(operand, pltpu.HBM)
            for operand in (
                impedance[0, 0],
                incident[0, 0],
                face_order[0],
                near_tiles[0, 0],
                basis_right[0, 0],
                rank_scale,
                rank_counts,
                coupling[0],
                basis_left[0, 0],
            )
        ]
    )
    return out[None, None]


def solution(mesh):
    placed = (
        P("sub", "grp", None, None),
        P("sub", "grp", None, None),
        P("sub", "grp", None),
        P("sub", "grp", None, None, None),
        P("sub", "grp", None, None),
        P("sub", None),
        P(),
        P("sub", None, None, None),
        P("sub", "grp", None, None),
    )
    two = mesh.shape["sub"] == 2 * QUARTERS
    body = functools.partial(two_layers, mesh.shape["grp"]) if two else per_device
    return jax.shard_map(
        body,
        mesh=mesh,
        in_specs=placed,
        out_specs=P("sub", "grp", None, None),
        check_vma=False,
    )
```

```python
import functools
import jax
import jax.numpy as jnp
from jax import lax
from jax.experimental import pallas as pl
from jax.experimental.pallas import tpu as pltpu
from jax.sharding import PartitionSpec as P

FACE_Q = 192
ITERS = 3


def from_partner(value, axis, distance):
    mask = 2**distance
    pairs = [(source, source ^ mask) for source in range(lax.axis_size(axis))]
    return lax.ppermute(value, axis, pairs)


def shifted(value, axis, steps):
    count = lax.axis_size(axis)
    first, last = (max(0, -steps), min(count, count - steps))
    return lax.ppermute(value, axis, [(source, source + steps) for source in range(first, last)])


def per_device(
    impedance,
    incident,
    face_order,
    near_tiles,
    basis_right,
    rank_scale,
    rank_counts,
    coupling,
    basis_left,
):
    z_cols = impedance[0, 0]
    source = incident[0, 0]
    order_map = face_order[0, 0]
    tiles = near_tiles[0, 0]
    right_basis = basis_right[0, 0]
    left_basis = basis_left[0, 0]
    couple_rows = coupling[0]
    position = lax.axis_index("sub")
    cluster = position // 4
    rank_ids = jnp.arange(rank_scale.shape[1])
    kept = jnp.where(rank_ids < rank_counts[cluster], rank_scale[0], jnp.float32(0.0))
    trace_now = source
    for sweep_index in range(ITERS):
        whole = trace_now
        for bit_number in (0, 1):
            partner = from_partner(whole, "sub", bit_number)
            upper_half = position // (1 << bit_number) % 2 == 1
            whole = jnp.where(
                upper_half,
                jnp.concatenate([partner, whole], 1),
                jnp.concatenate([whole, partner], 1),
            )
        outgoing = jnp.dot(whole, z_cols, preferred_element_type=jnp.float32).astype(jnp.bfloat16)
        lower_out = outgoing[:, :FACE_Q]
        upper_out = outgoing[:, FACE_Q : 2 * FACE_Q]
        outer_out = outgoing[:, 2 * FACE_Q :]
        partial_sum = jnp.dot(outer_out, right_basis, preferred_element_type=jnp.float32)
        total = lax.psum(partial_sum.astype(jnp.bfloat16), "grp").astype(jnp.float32)
        coefs = (total * kept).astype(jnp.bfloat16)
        block_rows = lax.all_gather(coefs[None], "sub", axis=0, tiled=True)
        sources = jnp.arange(block_rows.shape[0]) // 4
        chosen = jnp.take(couple_rows, sources, axis=0)
        chosen = jnp.where((sources != cluster)[:, None, None], chosen, jnp.zeros_like(chosen))
        far = jnp.einsum(
            "nkr,nrt->kt", block_rows, chosen, preferred_element_type=jnp.float32
        ).astype(jnp.bfloat16)
        arrived = []
        for offset in (4, -4):
            sent = (upper_out, outer_out) if offset > 0 else (lower_out, outer_out)
            arrived.append(shifted((sent[0], sent[1]), "sub", offset))
        upper_below, outer_below = arrived[0]
        lower_above, outer_above = arrived[1]
        lower_in = jnp.take(upper_below, order_map, axis=1)
        outer_in = jnp.dot(outer_out, tiles[0], preferred_element_type=jnp.float32)
        outer_in = outer_in + jnp.dot(outer_below, tiles[1], preferred_element_type=jnp.float32)
        outer_in = outer_in + jnp.dot(outer_above, tiles[2], preferred_element_type=jnp.float32)
        outer_in = outer_in + jnp.dot(far, left_basis, preferred_element_type=jnp.float32)
        joined = jnp.concatenate(
            [lower_in.astype(jnp.float32), lower_above.astype(jnp.float32), outer_in], 1
        )
        trace_now = (joined + source.astype(jnp.float32)).astype(jnp.bfloat16)
    return trace_now[None, None]


QUARTERS = 4
F32 = jnp.float32
BF16 = jnp.bfloat16


def dot(a, b):
    return jnp.dot(a, b, preferred_element_type=F32)


def two_layer_kernel(
    groups,
    z_hbm,
    inc_hbm,
    order_hbm,
    tiles_hbm,
    right_hbm,
    scale_hbm,
    counts_hbm,
    couple_hbm,
    left_hbm,
    out_ref,
    own_ref,
    cross_ref,
    cross_there,
    right_ref,
    scale_ref,
    counts_ref,
    couple_ref,
    left_ref,
    z_ref,
    inc_all,
    order_all,
    left_all,
    all_w,
    g_all,
    base,
    mine,
    sourced,
    owned,
    other,
    plane_sum,
    other_sum,
    z_sem,
    load_sem,
    const_send,
    const_recv,
    send,
    recv,
    far_send,
    far_recv,
    g_send,
    g_recv,
    cross_send,
    cross_recv,
    slab_sem,
    ready_sem,
    go_sem,
):
    sub = lax.axis_index("sub")
    grp = lax.axis_index("grp")
    layer = sub // QUARTERS
    q = sub % QUARTERS
    exc, width = inc_all.shape[1:]
    half = exc // 2
    rank = right_ref.shape[1]
    outer = own_ref.shape[1]
    face = order_all.shape[2]
    upper = layer == 1
    flip0 = sub + 1 - 2 * (sub % 2)
    flip1 = sub + 2 - 4 * ((sub // 2) % 2)
    flip01 = flip1 + 1 - 2 * (flip1 % 2)
    flip2 = sub + 4 - 8 * layer
    flip12 = flip1 + 4 - 8 * layer
    q1 = flip0 % QUARTERS
    q2 = flip1 % QUARTERS
    q3 = flip01 % QUARTERS

    def remote(src, dst, send_sem, recv_sem, to_sub, to_grp=None):
        return pltpu.make_async_remote_copy(
            src_ref=src,
            dst_ref=dst,
            send_sem=send_sem,
            recv_sem=recv_sem,
            device_id=(to_sub, grp if to_grp is None else to_grp),
            device_id_type=pl.DeviceIdType.MESH,
        )

    def signal(sem, to_sub, to_grp):
        pl.semaphore_signal(
            sem, inc=1, device_id=(to_sub, to_grp), device_id_type=pl.DeviceIdType.MESH
        )

    loads = {}
    for i, (name, src, dst) in enumerate(
        [
            ("inc", inc_hbm, inc_all.at[q]),
            ("right", right_hbm, right_ref),
            ("scale", scale_hbm, scale_ref),
            ("counts", counts_hbm, counts_ref),
            ("couple", couple_hbm, couple_ref),
            ("left", left_hbm, left_ref),
            ("own", tiles_hbm.at[0], own_ref),
            ("cross", tiles_hbm.at[2 - layer], cross_ref),
            ("order", order_hbm, order_all.at[q]),
        ]
    ):
        loads[name] = pltpu.make_async_copy(src, dst, load_sem.at[i])
        loads[name].start()
    z_copies = []
    for part in range(QUARTERS):
        rows = pl.ds(part * width, width)
        copy = pltpu.make_async_copy(z_hbm.at[rows], z_ref.at[rows], z_sem.at[part])
        copy.start()
        z_copies.append(copy)

    slab = 2 * QUARTERS
    lead = sub == 0
    barrier = pltpu.get_barrier_semaphore()

    @pl.when(lead)
    def _():
        for i in range(1, slab):
            signal(barrier, i, grp)
        for d in range(1, groups):
            signal(barrier, sub, lax.rem(grp + d, groups))

    @pl.when(jnp.logical_not(lead))
    def _():
        for i in range(1, slab - 1):
            signal(barrier, 1 + lax.rem(sub - 1 + i, slab - 1), grp)
        pl.semaphore_wait(barrier, slab - 1)
        signal(slab_sem, 0, grp)

    @pl.when(lead)
    def _():
        pl.semaphore_wait(slab_sem, slab - 1)

    pending = []
    buffers = [inc_all, left_all, order_all]
    firsts = {}

    def const_start(i):
        buf = buffers[i]
        a = remote(buf.at[q], buf.at[q], const_send.at[i, 0], const_recv.at[i, 0], flip1)
        b = remote(buf.at[q], buf.at[q], const_send.at[i, 1], const_recv.at[i, 1], flip0)
        a.start()
        b.start()
        firsts[i] = (a, b)
        pending.extend([a, b])

    def const_forward(i):
        buf = buffers[i]
        firsts[i][0].wait_recv()
        c = remote(buf.at[q2], buf.at[q2], const_send.at[i, 2], const_recv.at[i, 2], flip0)
        c.start()
        pending.append(c)
        return c

    loads["inc"].wait()
    cut = exc * 1 // 2 // 16 * 16
    head = inc_all.at[q, pl.ds(0, cut)]
    tail = inc_all.at[q, pl.ds(cut, exc - cut)]
    inc_x = remote(head, head, const_send.at[0, 0], const_recv.at[0, 0], flip1)
    inc_c = remote(inc_all.at[q], inc_all.at[q], const_send.at[0, 1], const_recv.at[0, 1], flip0)
    inc_tx = remote(tail, tail, const_send.at[3, 0], const_recv.at[3, 0], flip1)
    inc_td = remote(tail, tail, const_send.at[3, 1], const_recv.at[3, 1], flip01)
    for copy in (inc_x, inc_c, inc_td, inc_tx):
        copy.start()
        pending.append(copy)

    loads["cross"].wait()
    cross_copy = remote(cross_ref, cross_there, cross_send, cross_recv, flip2)
    cross_copy.start()
    pending.append(cross_copy)
    for name in ("right", "scale", "counts", "couple", "left", "own", "order"):
        loads[name].wait()
    lanes = lax.broadcasted_iota(jnp.int32, (1, rank), 1)
    kept = jnp.where(lanes < counts_ref[layer], scale_ref[...], F32(0.0))
    right_ref[...] = (right_ref[...].astype(F32) * kept).astype(BF16)
    left_all[q] = dot(couple_ref[1 - layer], left_ref[...]).astype(BF16)

    @pl.when(lead)
    def _():
        pl.semaphore_wait(barrier, groups - 1)
        for d in range(1, groups):
            signal(ready_sem, sub, lax.rem(grp + d, groups))

    for copy in z_copies:
        copy.wait()

    def z_quarter(index):
        return z_ref[pl.ds(pl.multiple_of(index * width, width), width), :]

    acc = dot(inc_all[q], z_quarter(q))
    inc_c.wait_recv()
    acc = acc + dot(inc_all[q1], z_quarter(q1))
    for i in (1, 2):
        const_start(i)

    @pl.when(lead)
    def _():
        pl.semaphore_wait(ready_sem, groups - 1)
        for i in range(1, slab):
            signal(go_sem, i, grp)

    inc_x.wait_recv()
    moved = inc_all.at[q2, pl.ds(0, cut)]
    fwd = remote(moved, moved, const_send.at[0, 2], const_recv.at[0, 2], flip0)
    fwd.start()
    pending.append(fwd)
    inc_tx.wait_recv()
    acc = acc + dot(inc_all[q2], z_quarter(q2))
    inc_td.wait_recv()
    fwd.wait_recv()
    acc = acc + dot(inc_all[q3], z_quarter(q3))
    base[...] = acc

    lane = lax.broadcasted_iota(jnp.int32, (half, outer), 1)
    low = lane < outer // 2
    first_here = low == upper
    first_there = low != upper
    slot = lax.broadcasted_iota(jnp.int32, (2 * outer, 2 * face), 0)
    in_half = slot % (outer // 2)
    full_entry = jnp.where(upper, slot + outer // 2, slot)
    half_entry = jnp.where(upper, in_half, in_half + outer)
    entry = jnp.where(slot < outer, full_entry, half_entry)
    along = lax.broadcasted_iota(jnp.int32, (1, face), 1)
    nothing = jnp.full((1, face), -1, jnp.int32)
    far_at = 3 * QUARTERS * outer

    def chosen(order_row):
        below = jnp.where(upper, order_row, nothing)
        above = jnp.where(upper, nothing, along)
        wanted = jnp.concatenate([below, above], 1)
        return jnp.where(entry == wanted, F32(1.0), F32(0.0)).astype(BF16)

    def face_tiles(block):
        full = block[exc : 2 * exc]
        packed = block[2 * exc : 2 * exc + half]
        zero = jnp.zeros_like(packed)
        top = jnp.where(first_there, packed, zero)
        bottom = jnp.where(first_there, zero, packed)
        return jnp.concatenate([full, jnp.concatenate([top, bottom], 0)], 1)

    def weights():
        for part in range(QUARTERS):
            start, at = part * width, 3 * part * outer
            z_outer = z_ref[start + 2 * face : start + width, :]
            all_w[at : at + outer, :] = z_outer
            term = dot(left_all[part], z_outer)
            total = term if part == 0 else total + term
            z_face = z_ref[start : start + 2 * face, :]
            all_w[at + outer : at + 3 * outer, :] = dot(chosen(order_all[part]), z_face).astype(BF16)
        all_w[far_at : far_at + rank, :] = total.astype(BF16)

    def to_plane(buf, sweep, first_sem, value):
        buf[sweep, q] = value.astype(BF16)
        at = buf.at[sweep, q]
        copies = []
        for sem, peer in ((first_sem, flip01), (first_sem + 1, flip1), (first_sem + 2, flip0)):
            copy = remote(at, at, send.at[sweep, sem], recv.at[sweep, sem], peer)
            copy.start()
            copies.append(copy)
            pending.append(copy)
        return copies[::-1]

    def start_source(sweep, outer_out):
        return to_plane(sourced, sweep, 2, dot(outer_out, right_ref[...]))

    def start_own(sweep, outer_out):
        owned[sweep, q] = dot(outer_out, own_ref[...]).astype(BF16)
        at = owned.at[sweep, q]
        ss, rs = send.at[sweep], recv.at[sweep]
        v_x = remote(at, at, ss.at[8], rs.at[8], flip1)
        v_c = remote(at, at, ss.at[9], rs.at[9], flip0)
        v_x.start()
        v_c.start()
        pending.extend([v_x, v_c])
        return v_c, v_x

    def forward_own(sweep, own):
        own[1].wait_recv()
        at = owned.at[sweep, q2]
        v_f = remote(at, at, send.at[sweep, 7], recv.at[sweep, 7], flip0)
        v_f.start()
        pending.append(v_f)
        return v_f

    def start_near(sweep, acc):
        ss, rs = send.at[sweep], recv.at[sweep]
        mid = acc[:, outer : 2 * outer]
        rolled = pltpu.roll(mid, outer // 2, 1)
        crossed = dot(acc[:, 2 * face :].astype(BF16), cross_there[...])
        mine[sweep, 0:exc] = crossed.astype(BF16)
        mine[sweep, exc : 2 * exc] = jnp.where(upper, acc[:, 0:outer], acc[:, 2 * outer : 3 * outer]).astype(BF16)
        mine[sweep, 2 * exc : 2 * exc + half] = jnp.where(first_here, mid[:half], rolled[half:]).astype(BF16)
        w_y = remote(mine.at[sweep], other.at[sweep, q], ss.at[0], rs.at[0], flip2)
        copies = [w_y]
        if sweep < ITERS - 1:
            copies.append(remote(mine.at[sweep], other.at[sweep, q], ss.at[1], rs.at[1], flip12))
        for copy in copies:
            copy.start()
            pending.append(copy)
        return copies

    def start_sums(sweep, value):
        plane_sum[sweep] = value.astype(BF16)
        sums = []
        for d in range(groups - 1, -1, -1):
            copy = remote(
                plane_sum.at[sweep],
                other_sum.at[sweep, d],
                far_send.at[sweep, d],
                far_recv.at[sweep, d],
                flip2,
                lax.rem(grp + d, groups),
            )
            copy.start()
            sums.append(copy)
            pending.append(copy)
        return sums

    def far_total(sweep, sums):
        for copy in sums:
            copy.wait_recv()
        total = other_sum[sweep, 0].astype(F32)
        for d in range(1, groups):
            total = total + other_sum[sweep, d].astype(F32)
        return total.astype(BF16)

    def near_block(sweep, part):
        block = other[sweep, part]
        outer_in = owned[sweep, part].astype(F32) + block[:exc].astype(F32)
        return jnp.concatenate([outer_in.astype(BF16), face_tiles(block)], 1)

    def near_rows(part):
        at = pl.multiple_of(3 * part * outer, outer)
        return all_w[pl.ds(at, 3 * outer), :]

    def known_terms(sweep, near, own):
        w_y, w_d = near
        ss, rs = send.at[sweep], recv.at[sweep]
        y_f = remote(other.at[sweep, q], other.at[sweep, q], ss.at[5], rs.at[5], flip0)
        d_f = remote(other.at[sweep, q2], other.at[sweep, q2], ss.at[6], rs.at[6], flip0)
        pending.extend([y_f, d_f])
        w_y.wait_recv()
        y_f.start()
        v_f = forward_own(sweep, own)
        known = base[...] + dot(near_block(sweep, q), near_rows(q))
        w_d.wait_recv()
        d_f.start()
        known = known + dot(near_block(sweep, q2), near_rows(q2))
        own[0].wait_recv()
        y_f.wait_recv()
        known = known + dot(near_block(sweep, q1), near_rows(q1))
        v_f.wait_recv()
        d_f.wait_recv()
        block, rows = near_block(sweep, q3), near_rows(q3)
        known_outer = known[:, 2 * face :] + dot(block, rows[:, 2 * face :])
        ahead = None
        if sweep == ITERS - 2:
            ahead = start_source(sweep + 1, known_outer.astype(BF16))
        known_face = known[:, : 2 * face] + dot(block, rows[:, : 2 * face])
        return jnp.concatenate([known_face, known_outer], 1), ahead

    for sweep in range(ITERS):
        last = sweep == ITERS - 1
        outer_out = acc[:, 2 * face :].astype(BF16)
        if sweep == 0:
            outs = start_source(sweep, outer_out)
            cross_copy.wait_recv()
            near = start_near(sweep, acc)
            own = start_own(sweep, outer_out)
            consts = [const_forward(1), const_forward(2)]
        elif not last:
            outs = start_source(sweep, outer_out)
            near = start_near(sweep, acc)
            own = start_own(sweep, outer_out)
        else:
            near = start_near(sweep, acc)
            outs = ahead
        if last:
            for copy in shares:
                copy.wait_recv()
            whole = g_all[0].astype(F32)
            for part in range(1, QUARTERS):
                whole = whole + g_all[part].astype(F32)
            value = dot(total, whole.astype(BF16))
        for copy in outs:
            copy.wait_recv()
        for part in range(QUARTERS):
            term = sourced[sweep, part].astype(F32)
            value = value + term if last or part else term
        if sweep == 0:

            @pl.when(jnp.logical_not(lead))
            def _():
                pl.semaphore_wait(go_sem, 1)

        sums = start_sums(sweep, value)
        if sweep == 0:
            for i in (1, 2):
                firsts[i][1].wait_recv()
            for c in consts:
                c.wait_recv()
            weights()
            far_outer = all_w[far_at : far_at + rank, 2 * face :]
            g_all[q] = dot(far_outer, right_ref[...]).astype(BF16)
            shares = [
                remote(g_all.at[q], g_all.at[q], g_send.at[i], g_recv.at[i], peer)
                for i, peer in enumerate((flip01, flip1, flip0))
            ]
            for copy in shares:
                copy.start()
                pending.append(copy)
        if not last:
            known, ahead = known_terms(sweep, near, own)
            total = far_total(sweep, sums)
            acc = known + dot(total, all_w[far_at : far_at + rank, :])
        else:
            near[0].wait_recv()
            block = other[sweep, q]
            outer_in = dot(outer_out, own_ref[...]) + block[:exc].astype(F32)
            faces = dot(face_tiles(block), chosen(order_all[q]))
            inc = inc_all[q].astype(F32)
            out_ref[:, 0 : 2 * face] = (faces + inc[:, : 2 * face]).astype(BF16)
            outer_in = outer_in + inc[:, 2 * face :]
            total = far_total(sweep, sums)
            outer_in = outer_in + dot(total, left_all[q])
            out_ref[:, 2 * face :] = outer_in.astype(BF16)
    for copy in pending:
        copy.wait_send()


def two_layers(
    groups,
    impedance,
    incident,
    face_order,
    near_tiles,
    basis_right,
    rank_scale,
    rank_counts,
    coupling,
    basis_left,
):
    order, width = impedance.shape[2:]
    exc = incident.shape[2]
    face = face_order.shape[2]
    outer = near_tiles.shape[3]
    rank = basis_right.shape[3]
    vmem = pl.BlockSpec(memory_space=pltpu.VMEM)
    dma = pltpu.SemaphoreType.DMA
    block = 2 * exc + exc // 2
    out = pl.pallas_call(
        functools.partial(two_layer_kernel, groups),
        out_shape=jax.ShapeDtypeStruct((exc, width), BF16),
        in_specs=[pl.BlockSpec(memory_space=pltpu.HBM)] * 9,
        out_specs=vmem,
        scratch_shapes=[
            pltpu.VMEM((outer, outer), BF16),
            pltpu.VMEM((outer, outer), BF16),
            pltpu.VMEM((outer, outer), BF16),
            pltpu.VMEM((outer, rank), BF16),
            pltpu.VMEM((1, rank), F32),
            pltpu.SMEM(rank_counts.shape, jnp.int32),
            pltpu.VMEM(coupling.shape[1:], BF16),
            pltpu.VMEM((rank, outer), BF16),
            pltpu.VMEM((order, width), BF16),
            pltpu.VMEM((QUARTERS, exc, width), BF16),
            pltpu.VMEM((QUARTERS, 1, face), jnp.int32),
            pltpu.VMEM((QUARTERS, rank, outer), BF16),
            pltpu.VMEM((3 * QUARTERS * outer + rank, width), BF16),
            pltpu.VMEM((QUARTERS, rank, rank), BF16),
            pltpu.VMEM((exc, width), F32),
            pltpu.VMEM((ITERS, block, outer), BF16),
            pltpu.VMEM((ITERS, QUARTERS, exc, rank), BF16),
            pltpu.VMEM((ITERS, QUARTERS, exc, outer), BF16),
            pltpu.VMEM((ITERS, QUARTERS, block, outer), BF16),
            pltpu.VMEM((ITERS, exc, rank), BF16),
            pltpu.VMEM((ITERS, groups, exc, rank), BF16),
            dma((QUARTERS,)),
            dma((9,)),
            dma((4, 3)),
            dma((4, 3)),
            dma((ITERS, 10)),
            dma((ITERS, 10)),
            dma((ITERS, groups)),
            dma((ITERS, groups)),
            dma((3,)),
            dma((3,)),
            dma,
            dma,
            pltpu.SemaphoreType.REGULAR,
            pltpu.SemaphoreType.REGULAR,
            pltpu.SemaphoreType.REGULAR,
        ],
        compiler_params=pltpu.CompilerParams(
            collective_id=0, has_side_effects=True, vmem_limit_bytes=48 * 1024 * 1024
        ),
    )(
        *[
            pltpu.with_memory_space_constraint(operand, pltpu.HBM)
            for operand in (
                impedance[0, 0],
                incident[0, 0],
                face_order[0],
                near_tiles[0, 0],
                basis_right[0, 0],
                rank_scale,
                rank_counts,
                coupling[0],
                basis_left[0, 0],
            )
        ]
    )
    return out[None, None]


def solution(mesh):
    placed = (
        P("sub", "grp", None, None),
        P("sub", "grp", None, None),
        P("sub", "grp", None),
        P("sub", "grp", None, None, None),
        P("sub", "grp", None, None),
        P("sub", None),
        P(),
        P("sub", None, None, None),
        P("sub", "grp", None, None),
    )
    two = mesh.shape["sub"] == 2 * QUARTERS
    body = functools.partial(two_layers, mesh.shape["grp"]) if two else per_device
    return jax.shard_map(
        body,
        mesh=mesh,
        in_specs=placed,
        out_specs=P("sub", "grp", None, None),
        check_vma=False,
    )
```

```python
import functools
import jax
import jax.numpy as jnp
from jax import lax
from jax.experimental import pallas as pl
from jax.experimental.pallas import tpu as pltpu
from jax.sharding import PartitionSpec as P

FACE_Q = 192
ITERS = 3


def from_partner(value, axis, distance):
    mask = 2**distance
    pairs = [(source, source ^ mask) for source in range(lax.axis_size(axis))]
    return lax.ppermute(value, axis, pairs)


def shifted(value, axis, steps):
    count = lax.axis_size(axis)
    first, last = (max(0, -steps), min(count, count - steps))
    return lax.ppermute(value, axis, [(source, source + steps) for source in range(first, last)])


def per_device(
    impedance,
    incident,
    face_order,
    near_tiles,
    basis_right,
    rank_scale,
    rank_counts,
    coupling,
    basis_left,
):
    z_cols = impedance[0, 0]
    source = incident[0, 0]
    order_map = face_order[0, 0]
    tiles = near_tiles[0, 0]
    right_basis = basis_right[0, 0]
    left_basis = basis_left[0, 0]
    couple_rows = coupling[0]
    position = lax.axis_index("sub")
    cluster = position // 4
    rank_ids = jnp.arange(rank_scale.shape[1])
    kept = jnp.where(rank_ids < rank_counts[cluster], rank_scale[0], jnp.float32(0.0))
    trace_now = source
    for sweep_index in range(ITERS):
        whole = trace_now
        for bit_number in (0, 1):
            partner = from_partner(whole, "sub", bit_number)
            upper_half = position // (1 << bit_number) % 2 == 1
            whole = jnp.where(
                upper_half,
                jnp.concatenate([partner, whole], 1),
                jnp.concatenate([whole, partner], 1),
            )
        outgoing = jnp.dot(whole, z_cols, preferred_element_type=jnp.float32).astype(jnp.bfloat16)
        lower_out = outgoing[:, :FACE_Q]
        upper_out = outgoing[:, FACE_Q : 2 * FACE_Q]
        outer_out = outgoing[:, 2 * FACE_Q :]
        partial_sum = jnp.dot(outer_out, right_basis, preferred_element_type=jnp.float32)
        total = lax.psum(partial_sum.astype(jnp.bfloat16), "grp").astype(jnp.float32)
        coefs = (total * kept).astype(jnp.bfloat16)
        block_rows = lax.all_gather(coefs[None], "sub", axis=0, tiled=True)
        sources = jnp.arange(block_rows.shape[0]) // 4
        chosen = jnp.take(couple_rows, sources, axis=0)
        chosen = jnp.where((sources != cluster)[:, None, None], chosen, jnp.zeros_like(chosen))
        far = jnp.einsum(
            "nkr,nrt->kt", block_rows, chosen, preferred_element_type=jnp.float32
        ).astype(jnp.bfloat16)
        arrived = []
        for offset in (4, -4):
            sent = (upper_out, outer_out) if offset > 0 else (lower_out, outer_out)
            arrived.append(shifted((sent[0], sent[1]), "sub", offset))
        upper_below, outer_below = arrived[0]
        lower_above, outer_above = arrived[1]
        lower_in = jnp.take(upper_below, order_map, axis=1)
        outer_in = jnp.dot(outer_out, tiles[0], preferred_element_type=jnp.float32)
        outer_in = outer_in + jnp.dot(outer_below, tiles[1], preferred_element_type=jnp.float32)
        outer_in = outer_in + jnp.dot(outer_above, tiles[2], preferred_element_type=jnp.float32)
        outer_in = outer_in + jnp.dot(far, left_basis, preferred_element_type=jnp.float32)
        joined = jnp.concatenate(
            [lower_in.astype(jnp.float32), lower_above.astype(jnp.float32), outer_in], 1
        )
        trace_now = (joined + source.astype(jnp.float32)).astype(jnp.bfloat16)
    return trace_now[None, None]


QUARTERS = 4
F32 = jnp.float32
BF16 = jnp.bfloat16


def dot(a, b):
    return jnp.dot(a, b, preferred_element_type=F32)


def two_layer_kernel(
    groups,
    z_hbm,
    inc_hbm,
    order_hbm,
    tiles_hbm,
    right_hbm,
    scale_hbm,
    counts_hbm,
    couple_hbm,
    left_hbm,
    out_ref,
    own_ref,
    cross_ref,
    cross_there,
    right_ref,
    scale_ref,
    counts_ref,
    couple_ref,
    left_ref,
    z_ref,
    inc_all,
    order_all,
    left_all,
    all_w,
    g_all,
    base,
    mine,
    sourced,
    owned,
    other,
    plane_sum,
    other_sum,
    z_sem,
    load_sem,
    const_send,
    const_recv,
    send,
    recv,
    far_send,
    far_recv,
    g_send,
    g_recv,
    cross_send,
    cross_recv,
    slab_sem,
    ready_sem,
    go_sem,
):
    sub = lax.axis_index("sub")
    grp = lax.axis_index("grp")
    layer = sub // QUARTERS
    q = sub % QUARTERS
    exc, width = inc_all.shape[1:]
    half = exc // 2
    rank = right_ref.shape[1]
    outer = own_ref.shape[1]
    face = order_all.shape[2]
    upper = layer == 1
    flip0 = sub + 1 - 2 * (sub % 2)
    flip1 = sub + 2 - 4 * ((sub // 2) % 2)
    flip01 = flip1 + 1 - 2 * (flip1 % 2)
    flip2 = sub + 4 - 8 * layer
    flip12 = flip1 + 4 - 8 * layer
    q1 = flip0 % QUARTERS
    q2 = flip1 % QUARTERS
    q3 = flip01 % QUARTERS

    def remote(src, dst, send_sem, recv_sem, to_sub, to_grp=None):
        return pltpu.make_async_remote_copy(
            src_ref=src,
            dst_ref=dst,
            send_sem=send_sem,
            recv_sem=recv_sem,
            device_id=(to_sub, grp if to_grp is None else to_grp),
            device_id_type=pl.DeviceIdType.MESH,
        )

    def signal(sem, to_sub, to_grp):
        pl.semaphore_signal(
            sem, inc=1, device_id=(to_sub, to_grp), device_id_type=pl.DeviceIdType.MESH
        )

    loads = {}
    for i, (name, src, dst) in enumerate(
        [
            ("inc", inc_hbm, inc_all.at[q]),
            ("right", right_hbm, right_ref),
            ("scale", scale_hbm, scale_ref),
            ("counts", counts_hbm, counts_ref),
            ("couple", couple_hbm, couple_ref),
            ("left", left_hbm, left_ref),
            ("own", tiles_hbm.at[0], own_ref),
            ("cross", tiles_hbm.at[2 - layer], cross_ref),
            ("order", order_hbm, order_all.at[q]),
        ]
    ):
        loads[name] = pltpu.make_async_copy(src, dst, load_sem.at[i])
        loads[name].start()
    z_copies = []
    for part in range(QUARTERS):
        rows = pl.ds(part * width, width)
        copy = pltpu.make_async_copy(z_hbm.at[rows], z_ref.at[rows], z_sem.at[part])
        copy.start()
        z_copies.append(copy)

    slab = 2 * QUARTERS
    lead = sub == 0
    barrier = pltpu.get_barrier_semaphore()

    @pl.when(lead)
    def _():
        for i in range(1, slab):
            signal(barrier, i, grp)
        for d in range(1, groups):
            signal(barrier, sub, lax.rem(grp + d, groups))

    @pl.when(jnp.logical_not(lead))
    def _():
        for i in range(1, slab - 1):
            signal(barrier, 1 + lax.rem(sub - 1 + i, slab - 1), grp)
        pl.semaphore_wait(barrier, slab - 1)
        signal(slab_sem, 0, grp)

    @pl.when(lead)
    def _():
        pl.semaphore_wait(slab_sem, slab - 1)

    pending = []
    buffers = [inc_all, left_all, order_all]
    firsts = {}

    def const_start(i):
        buf = buffers[i]
        a = remote(buf.at[q], buf.at[q], const_send.at[i, 0], const_recv.at[i, 0], flip1)
        b = remote(buf.at[q], buf.at[q], const_send.at[i, 1], const_recv.at[i, 1], flip0)
        a.start()
        b.start()
        firsts[i] = (a, b)
        pending.extend([a, b])

    def const_forward(i):
        buf = buffers[i]
        firsts[i][0].wait_recv()
        c = remote(buf.at[q2], buf.at[q2], const_send.at[i, 2], const_recv.at[i, 2], flip0)
        c.start()
        pending.append(c)
        return c

    loads["inc"].wait()
    cut = exc * 1 // 2 // 16 * 16
    head = inc_all.at[q, pl.ds(0, cut)]
    tail = inc_all.at[q, pl.ds(cut, exc - cut)]
    inc_x = remote(head, head, const_send.at[0, 0], const_recv.at[0, 0], flip1)
    inc_c = remote(inc_all.at[q], inc_all.at[q], const_send.at[0, 1], const_recv.at[0, 1], flip0)
    inc_tx = remote(tail, tail, const_send.at[3, 0], const_recv.at[3, 0], flip1)
    inc_td = remote(tail, tail, const_send.at[3, 1], const_recv.at[3, 1], flip01)
    for copy in (inc_x, inc_c, inc_td, inc_tx):
        copy.start()
        pending.append(copy)

    loads["cross"].wait()
    cross_copy = remote(cross_ref, cross_there, cross_send, cross_recv, flip2)
    cross_copy.start()
    pending.append(cross_copy)
    for name in ("right", "scale", "counts", "couple", "left", "own", "order"):
        loads[name].wait()
    lanes = lax.broadcasted_iota(jnp.int32, (1, rank), 1)
    kept = jnp.where(lanes < counts_ref[layer], scale_ref[...], F32(0.0))
    right_ref[...] = (right_ref[...].astype(F32) * kept).astype(BF16)
    left_all[q] = dot(couple_ref[1 - layer], left_ref[...]).astype(BF16)

    @pl.when(lead)
    def _():
        pl.semaphore_wait(barrier, groups - 1)
        for d in range(1, groups):
            signal(ready_sem, sub, lax.rem(grp + d, groups))

    for copy in z_copies:
        copy.wait()

    def z_quarter(index):
        return z_ref[pl.ds(pl.multiple_of(index * width, width), width), :]

    acc = dot(inc_all[q], z_quarter(q))
    inc_c.wait_recv()
    acc = acc + dot(inc_all[q1], z_quarter(q1))
    for i in (1, 2):
        const_start(i)

    @pl.when(lead)
    def _():
        pl.semaphore_wait(ready_sem, groups - 1)
        for i in range(1, slab):
            signal(go_sem, i, grp)

    inc_x.wait_recv()
    moved = inc_all.at[q2, pl.ds(0, cut)]
    fwd = remote(moved, moved, const_send.at[0, 2], const_recv.at[0, 2], flip0)
    fwd.start()
    pending.append(fwd)
    inc_tx.wait_recv()
    acc = acc + dot(inc_all[q2], z_quarter(q2))
    inc_td.wait_recv()
    fwd.wait_recv()
    acc = acc + dot(inc_all[q3], z_quarter(q3))
    base[...] = acc

    lane = lax.broadcasted_iota(jnp.int32, (half, outer), 1)
    low = lane < outer // 2
    first_here = low == upper
    first_there = low != upper
    slot = lax.broadcasted_iota(jnp.int32, (2 * outer, 2 * face), 0)
    in_half = slot % (outer // 2)
    full_entry = jnp.where(upper, slot + outer // 2, slot)
    half_entry = jnp.where(upper, in_half, in_half + outer)
    entry = jnp.where(slot < outer, full_entry, half_entry)
    along = lax.broadcasted_iota(jnp.int32, (1, face), 1)
    nothing = jnp.full((1, face), -1, jnp.int32)
    far_at = 3 * QUARTERS * outer

    def chosen(order_row):
        below = jnp.where(upper, order_row, nothing)
        above = jnp.where(upper, nothing, along)
        wanted = jnp.concatenate([below, above], 1)
        return jnp.where(entry == wanted, F32(1.0), F32(0.0)).astype(BF16)

    def face_tiles(block):
        full = block[exc : 2 * exc]
        packed = block[2 * exc : 2 * exc + half]
        zero = jnp.zeros_like(packed)
        top = jnp.where(first_there, packed, zero)
        bottom = jnp.where(first_there, zero, packed)
        return jnp.concatenate([full, jnp.concatenate([top, bottom], 0)], 1)

    def weights():
        for part in range(QUARTERS):
            start, at = part * width, 3 * part * outer
            z_outer = z_ref[start + 2 * face : start + width, :]
            all_w[at : at + outer, :] = z_outer
            term = dot(left_all[part], z_outer)
            total = term if part == 0 else total + term
            z_face = z_ref[start : start + 2 * face, :]
            all_w[at + outer : at + 3 * outer, :] = dot(chosen(order_all[part]), z_face).astype(BF16)
        all_w[far_at : far_at + rank, :] = total.astype(BF16)

    def to_plane(buf, sweep, first_sem, value):
        buf[sweep, q] = value.astype(BF16)
        at = buf.at[sweep, q]
        copies = []
        for sem, peer in ((first_sem, flip01), (first_sem + 1, flip1), (first_sem + 2, flip0)):
            copy = remote(at, at, send.at[sweep, sem], recv.at[sweep, sem], peer)
            copy.start()
            copies.append(copy)
            pending.append(copy)
        return copies[::-1]

    def start_source(sweep, outer_out):
        return to_plane(sourced, sweep, 2, dot(outer_out, right_ref[...]))

    def start_own(sweep, outer_out):
        owned[sweep, q] = dot(outer_out, own_ref[...]).astype(BF16)
        at = owned.at[sweep, q]
        ss, rs = send.at[sweep], recv.at[sweep]
        v_x = remote(at, at, ss.at[8], rs.at[8], flip1)
        v_c = remote(at, at, ss.at[9], rs.at[9], flip0)
        v_x.start()
        v_c.start()
        pending.extend([v_x, v_c])
        return v_c, v_x

    def forward_own(sweep, own):
        own[1].wait_recv()
        at = owned.at[sweep, q2]
        v_f = remote(at, at, send.at[sweep, 7], recv.at[sweep, 7], flip0)
        v_f.start()
        pending.append(v_f)
        return v_f

    def start_near(sweep, acc):
        ss, rs = send.at[sweep], recv.at[sweep]
        mid = acc[:, outer : 2 * outer]
        rolled = pltpu.roll(mid, outer // 2, 1)
        crossed = dot(acc[:, 2 * face :].astype(BF16), cross_there[...])
        mine[sweep, 0:exc] = crossed.astype(BF16)
        mine[sweep, exc : 2 * exc] = jnp.where(upper, acc[:, 0:outer], acc[:, 2 * outer : 3 * outer]).astype(BF16)
        mine[sweep, 2 * exc : 2 * exc + half] = jnp.where(first_here, mid[:half], rolled[half:]).astype(BF16)
        w_y = remote(mine.at[sweep], other.at[sweep, q], ss.at[0], rs.at[0], flip2)
        copies = [w_y]
        if sweep < ITERS - 1:
            copies.append(remote(mine.at[sweep], other.at[sweep, q], ss.at[1], rs.at[1], flip12))
        for copy in copies:
            copy.start()
            pending.append(copy)
        return copies

    def start_sums(sweep, value):
        plane_sum[sweep] = value.astype(BF16)
        sums = []
        for d in range(groups - 1, -1, -1):
            copy = remote(
                plane_sum.at[sweep],
                other_sum.at[sweep, d],
                far_send.at[sweep, d],
                far_recv.at[sweep, d],
                flip2,
                lax.rem(grp + d, groups),
            )
            copy.start()
            sums.append(copy)
            pending.append(copy)
        return sums

    def far_total(sweep, sums):
        for copy in sums:
            copy.wait_recv()
        total = other_sum[sweep, 0].astype(F32)
        for d in range(1, groups):
            total = total + other_sum[sweep, d].astype(F32)
        return total.astype(BF16)

    def near_block(sweep, part):
        block = other[sweep, part]
        outer_in = owned[sweep, part].astype(F32) + block[:exc].astype(F32)
        return jnp.concatenate([outer_in.astype(BF16), face_tiles(block)], 1)

    def near_rows(part):
        at = pl.multiple_of(3 * part * outer, outer)
        return all_w[pl.ds(at, 3 * outer), :]

    def known_terms(sweep, near, own):
        w_y, w_d = near
        ss, rs = send.at[sweep], recv.at[sweep]
        y_f = remote(other.at[sweep, q], other.at[sweep, q], ss.at[5], rs.at[5], flip0)
        d_f = remote(other.at[sweep, q2], other.at[sweep, q2], ss.at[6], rs.at[6], flip0)
        pending.extend([y_f, d_f])
        w_y.wait_recv()
        y_f.start()
        v_f = forward_own(sweep, own)
        known = base[...] + dot(near_block(sweep, q), near_rows(q))
        w_d.wait_recv()
        d_f.start()
        known = known + dot(near_block(sweep, q2), near_rows(q2))
        own[0].wait_recv()
        y_f.wait_recv()
        known = known + dot(near_block(sweep, q1), near_rows(q1))
        v_f.wait_recv()
        d_f.wait_recv()
        block, rows = near_block(sweep, q3), near_rows(q3)
        known_outer = known[:, 2 * face :] + dot(block, rows[:, 2 * face :])
        ahead = None
        if sweep == ITERS - 2:
            ahead = start_source(sweep + 1, known_outer.astype(BF16))
        known_face = known[:, : 2 * face] + dot(block, rows[:, : 2 * face])
        return jnp.concatenate([known_face, known_outer], 1), ahead

    for sweep in range(ITERS):
        last = sweep == ITERS - 1
        outer_out = acc[:, 2 * face :].astype(BF16)
        if sweep == 0:
            outs = start_source(sweep, outer_out)
            own = start_own(sweep, outer_out)
            cross_copy.wait_recv()
            near = start_near(sweep, acc)
            consts = [const_forward(1), const_forward(2)]
        elif not last:
            outs = start_source(sweep, outer_out)
            near = start_near(sweep, acc)
            own = start_own(sweep, outer_out)
        else:
            near = start_near(sweep, acc)
            outs = ahead
        if last:
            for copy in shares:
                copy.wait_recv()
            whole = g_all[0].astype(F32)
            for part in range(1, QUARTERS):
                whole = whole + g_all[part].astype(F32)
            value = dot(total, whole.astype(BF16))
        for copy in outs:
            copy.wait_recv()
        for part in range(QUARTERS):
            term = sourced[sweep, part].astype(F32)
            value = value + term if last or part else term
        if sweep == 0:

            @pl.when(jnp.logical_not(lead))
            def _():
                pl.semaphore_wait(go_sem, 1)

        sums = start_sums(sweep, value)
        if sweep == 0:
            for i in (1, 2):
                firsts[i][1].wait_recv()
            for c in consts:
                c.wait_recv()
            weights()
            far_outer = all_w[far_at : far_at + rank, 2 * face :]
            g_all[q] = dot(far_outer, right_ref[...]).astype(BF16)
            shares = [
                remote(g_all.at[q], g_all.at[q], g_send.at[i], g_recv.at[i], peer)
                for i, peer in enumerate((flip01, flip1, flip0))
            ]
            for copy in shares:
                copy.start()
                pending.append(copy)
        if not last:
            known, ahead = known_terms(sweep, near, own)
            total = far_total(sweep, sums)
            acc = known + dot(total, all_w[far_at : far_at + rank, :])
        else:
            near[0].wait_recv()
            block = other[sweep, q]
            outer_in = dot(outer_out, own_ref[...]) + block[:exc].astype(F32)
            faces = dot(face_tiles(block), chosen(order_all[q]))
            inc = inc_all[q].astype(F32)
            out_ref[:, 0 : 2 * face] = (faces + inc[:, : 2 * face]).astype(BF16)
            outer_in = outer_in + inc[:, 2 * face :]
            total = far_total(sweep, sums)
            outer_in = outer_in + dot(total, left_all[q])
            out_ref[:, 2 * face :] = outer_in.astype(BF16)
    for copy in pending:
        copy.wait_send()


def two_layers(
    groups,
    impedance,
    incident,
    face_order,
    near_tiles,
    basis_right,
    rank_scale,
    rank_counts,
    coupling,
    basis_left,
):
    order, width = impedance.shape[2:]
    exc = incident.shape[2]
    face = face_order.shape[2]
    outer = near_tiles.shape[3]
    rank = basis_right.shape[3]
    vmem = pl.BlockSpec(memory_space=pltpu.VMEM)
    dma = pltpu.SemaphoreType.DMA
    block = 2 * exc + exc // 2
    out = pl.pallas_call(
        functools.partial(two_layer_kernel, groups),
        out_shape=jax.ShapeDtypeStruct((exc, width), BF16),
        in_specs=[pl.BlockSpec(memory_space=pltpu.HBM)] * 9,
        out_specs=vmem,
        scratch_shapes=[
            pltpu.VMEM((outer, outer), BF16),
            pltpu.VMEM((outer, outer), BF16),
            pltpu.VMEM((outer, outer), BF16),
            pltpu.VMEM((outer, rank), BF16),
            pltpu.VMEM((1, rank), F32),
            pltpu.SMEM(rank_counts.shape, jnp.int32),
            pltpu.VMEM(coupling.shape[1:], BF16),
            pltpu.VMEM((rank, outer), BF16),
            pltpu.VMEM((order, width), BF16),
            pltpu.VMEM((QUARTERS, exc, width), BF16),
            pltpu.VMEM((QUARTERS, 1, face), jnp.int32),
            pltpu.VMEM((QUARTERS, rank, outer), BF16),
            pltpu.VMEM((3 * QUARTERS * outer + rank, width), BF16),
            pltpu.VMEM((QUARTERS, rank, rank), BF16),
            pltpu.VMEM((exc, width), F32),
            pltpu.VMEM((ITERS, block, outer), BF16),
            pltpu.VMEM((ITERS, QUARTERS, exc, rank), BF16),
            pltpu.VMEM((ITERS, QUARTERS, exc, outer), BF16),
            pltpu.VMEM((ITERS, QUARTERS, block, outer), BF16),
            pltpu.VMEM((ITERS, exc, rank), BF16),
            pltpu.VMEM((ITERS, groups, exc, rank), BF16),
            dma((QUARTERS,)),
            dma((9,)),
            dma((4, 3)),
            dma((4, 3)),
            dma((ITERS, 10)),
            dma((ITERS, 10)),
            dma((ITERS, groups)),
            dma((ITERS, groups)),
            dma((3,)),
            dma((3,)),
            dma,
            dma,
            pltpu.SemaphoreType.REGULAR,
            pltpu.SemaphoreType.REGULAR,
            pltpu.SemaphoreType.REGULAR,
        ],
        compiler_params=pltpu.CompilerParams(
            collective_id=0, has_side_effects=True, vmem_limit_bytes=48 * 1024 * 1024
        ),
    )(
        *[
            pltpu.with_memory_space_constraint(operand, pltpu.HBM)
            for operand in (
                impedance[0, 0],
                incident[0, 0],
                face_order[0],
                near_tiles[0, 0],
                basis_right[0, 0],
                rank_scale,
                rank_counts,
                coupling[0],
                basis_left[0, 0],
            )
        ]
    )
    return out[None, None]


def solution(mesh):
    placed = (
        P("sub", "grp", None, None),
        P("sub", "grp", None, None),
        P("sub", "grp", None),
        P("sub", "grp", None, None, None),
        P("sub", "grp", None, None),
        P("sub", None),
        P(),
        P("sub", None, None, None),
        P("sub", "grp", None, None),
    )
    two = mesh.shape["sub"] == 2 * QUARTERS
    body = functools.partial(two_layers, mesh.shape["grp"]) if two else per_device
    return jax.shard_map(
        body,
        mesh=mesh,
        in_specs=placed,
        out_specs=P("sub", "grp", None, None),
        check_vma=False,
    )
```
